256 devices in a mesh: blk: 16 (over z, y_lo), grp: 16 (over x, y_hi, core).
Axes of the slice: x: 4, y: 4 (y_hi: 2, y_lo: 2; y = y_hi * 2 + y_lo), z: 8, core: 2. Of those that a mesh axis runs over, the one named last changes fastest.
Arguments:
- frames: bfloat16 [16, 4096, 1024], P('grp', 'blk'), may hold values from -16 to 16
- utt_lengths: int32 [8], replicated, may hold values from 1 to 16384, 65536 in all
- attn_gain: float32 [1024], replicated, may hold values from 0.25 to 1.75
- w_qkv: bfloat16 [1024, 3072], P(None, 'grp'), may hold values from -4 to 4
- w_out: bfloat16 [1024, 1024], replicated, may hold values from -0.375 to 0.375
- conv_gain: float32 [1024], replicated, may hold values from 0.25 to 1.75
- w_glu: bfloat16 [1024, 2048], replicated, may hold values from -0.1875 to 0.1875
- w_depth: float32 [31, 1024], replicated, may hold values from -1 to 1
- depth_gain: float32 [1024], replicated, may hold values from 0.25 to 1.75
- w_proj: bfloat16 [1024, 1024], replicated, may hold values from -0.1875 to 0.1875
Outputs:
- block_out: bfloat16 [16, 4096, 1024], P('grp', 'blk')
The draws below stay inside these ranges and needn't reach their ends.
Inputs may be any that keep to these rules, and one draw needn't show every extreme that they name: `utt_lengths`: they sum to 65536 and the longest is exactly 16384.
All inputs are finite; a program needn't handle non-finite values.
Results may differ from the reference program's by a relative error of at most 0.0095.
Values may be sent and summed in bfloat16 or wider, within the bound.
No kernel may reach another device: no remote copies, remote signals or barrier semaphores. Data moves between devices by JAX's collectives and lax.ppermute only.
A program may use at most 192 MiB of HBM per device.

```python
import math
import jax
import jax.numpy as jnp
import numpy as np
from jax import lax

D = 1024
HEADS = 16
KERNEL = 31
WINDOW = 4096
GROUPS = 16
TOKENS = 65536
UTT_MOST = 16384
UTTERANCES = 8


def draw_frames(key, part):
    base_key = jax.random.fold_in(jax.random.fold_in(key, 11), 0)
    drawn = jax.random.normal(base_key, (GROUPS, WINDOW, D), jnp.float32)
    return jnp.clip(drawn, -16.0, 16.0).astype(jnp.bfloat16)


def draw_w_qkv(key, part):
    drawn = jax.random.normal(jax.random.fold_in(key, 23), (D, HEADS, 3, D // HEADS), jnp.float32) * (1.4 / math.sqrt(D))
    return jnp.clip(drawn.reshape(D, 3 * D), -4.0, 4.0).astype(jnp.bfloat16)


def length_profile(amount, total, most, slope):
    loads = [(1 << 20) // math.isqrt(grade ** slope) + 1 for grade in range(2, amount + 1)]
    surplus, counts = total - most - (amount - 1), [1] * (amount - 1)
    while surplus > 0:
        candidates = [i for i in range(amount - 1) if counts[i] < most]
        pool, remaining = sum([loads[i] for i in candidates]), surplus
        for i in candidates:
            addition = min(most - counts[i], max(1, remaining * loads[i] // pool), surplus)
            counts[i] = counts[i] + addition
            surplus = surplus - addition
    return np.array([most] + counts)


def ragged(own_key, count, total, reach, slope):
    if count == 2:
        one = jax.random.randint(own_key, (), max(1, total - reach), min(reach, total - 1) + 1)
        return jnp.stack([one, total - one])
    sizes = jnp.asarray(length_profile(count, total, reach, slope), jnp.int32)
    pairs = (count - 1) // 2
    donor, taker = sizes[1:1 + 2 * pairs:2], sizes[2:2 + 2 * pairs:2]
    slack = jnp.minimum(donor - 1, reach - taker)
    moved = jax.random.randint(jax.random.fold_in(own_key, 1), (pairs,), 0, 1 << 20) % (slack + 1)
    sizes = sizes.at[1:1 + 2 * pairs:2].set(donor - moved).at[2:2 + 2 * pairs:2].set(taker + moved)
    return sizes[jax.random.permutation(jax.random.fold_in(own_key, 2), count)]


def centred(stream_key, shape, scale, limit, held_as=jnp.bfloat16):
    values = scale * jax.random.normal(stream_key, shape, jnp.float32)
    return jnp.clip(values, min=-limit, max=limit).astype(held_as)


def setup_inputs(seed: int = 0) -> dict:
    splits = jax.random.split(jax.random.key(seed), 11)
    return {
        "frames": draw_frames(jax.random.fold_in(splits[10], 71), 0),
        "utt_lengths": ragged(splits[1], UTTERANCES, TOKENS, UTT_MOST, 2).astype(jnp.int32),
        "attn_gain": jnp.clip(1.0 + 0.15 * jax.random.normal(splits[2], (D,), jnp.float32), 0.25, 1.75),
        "w_qkv": draw_w_qkv(jax.random.fold_in(splits[10], 71), 0),
        "w_out": centred(splits[4], (D, D), (D // 4) ** -0.5, 0.375),
        "conv_gain": jnp.clip(1.0 + 0.15 * jax.random.normal(splits[5], (D,), jnp.float32), 0.25, 1.75),
        "w_glu": centred(splits[6], (D, 2 * D), D ** -0.5, 0.1875),
        "w_depth": centred(splits[7], (KERNEL, D), KERNEL ** -0.5, 1.0, jnp.float32),
        "depth_gain": jnp.clip(1.0 + 0.15 * jax.random.normal(splits[8], (D,), jnp.float32), 0.25, 1.75),
        "w_proj": centred(splits[9], (D, D), D ** -0.5, 0.1875),
    }


epsilon = 1e-05
big_negative = -1e+30

def normalize(values, row_gain):
    center = values - lax.optimization_barrier(jnp.mean(values, axis=-1, keepdims=True))
    spread = lax.optimization_barrier(jnp.mean(center * center, axis=-1, keepdims=True))
    return center * lax.rsqrt(spread + epsilon) * row_gain

def segment_of(utt_lengths, positions):
    starts = jnp.cumsum(utt_lengths) - utt_lengths
    started = (starts[None, :] <= positions[:, None]).astype(jnp.int32)
    return lax.optimization_barrier(jnp.sum(started, axis=1)) - 1

def one_head(head_qkv, seg_row, score_scale):
    scores = jnp.dot(head_qkv[0], head_qkv[1].T, preferred_element_type=jnp.float32) * score_scale
    allowed = seg_row[:, None] == seg_row[None, :]
    row_max = lax.optimization_barrier(jnp.max(jnp.where(allowed, scores, big_negative), axis=1, keepdims=True))
    weights = jnp.where(allowed, jnp.exp(scores - row_max), 0.0)
    row_total = lax.optimization_barrier(jnp.sum(weights, axis=1, keepdims=True))
    mixed_values = jnp.dot(weights.astype(jnp.bfloat16), head_qkv[2], preferred_element_type=jnp.float32)
    return mixed_values / row_total

def reference(frames, utt_lengths, attn_gain, w_qkv, w_out, conv_gain, w_glu, w_depth, depth_gain, w_proj):
    head_width = D // HEADS
    kernel_half = (KERNEL - 1) // 2
    score_scale = head_width ** (-0.5)
    flat_frames = frames.reshape(TOKENS, D)
    flat_float = flat_frames.astype(jnp.float32)
    frame_seg = segment_of(utt_lengths, jnp.arange(TOKENS, dtype=jnp.int32))
    normed = normalize(flat_float, attn_gain).astype(jnp.bfloat16)
    qkv_rows = jnp.dot(normed, w_qkv, preferred_element_type=jnp.float32).astype(jnp.bfloat16)
    arranged = jnp.transpose(qkv_rows.reshape(GROUPS, WINDOW, HEADS, 3, head_width), (0, 2, 3, 1, 4))
    group_seg = frame_seg.reshape(GROUPS, WINDOW)

    def one_group(operands):
        group_qkv, seg_row = operands
        return lax.map(lambda head_qkv: one_head(head_qkv, seg_row, score_scale), group_qkv)
    heads_out = lax.map(one_group, (arranged, group_seg))
    attended = jnp.transpose(heads_out, (0, 2, 1, 3)).reshape(TOKENS, D).astype(jnp.bfloat16)
    residual = (flat_float + jnp.dot(attended, w_out, preferred_element_type=jnp.float32)).astype(jnp.bfloat16)
    residual = lax.optimization_barrier(residual)
    conv_in = normalize(residual.astype(jnp.float32), conv_gain).astype(jnp.bfloat16)
    projected = jnp.dot(conv_in, w_glu, preferred_element_type=jnp.float32)
    gated = (projected[:, :D] * jax.nn.sigmoid(projected[:, D:])).astype(jnp.bfloat16)
    gated = lax.optimization_barrier(gated)
    padded = jnp.pad(gated.astype(jnp.float32), ((kernel_half, kernel_half), (0, 0)))
    pad_seg = segment_of(utt_lengths, jnp.arange(-kernel_half, TOKENS + kernel_half, dtype=jnp.int32))
    mixed_conv = jnp.zeros((TOKENS, D), jnp.float32)
    for offset in range(KERNEL):
        same_seg = (pad_seg[offset:offset + TOKENS] == frame_seg)[:, None]
        mixed_conv = mixed_conv + jnp.where(same_seg, padded[offset:offset + TOKENS] * w_depth[offset], 0.0)
    normed_conv = normalize(mixed_conv, depth_gain)
    activated = (normed_conv * jax.nn.sigmoid(normed_conv)).astype(jnp.bfloat16)
    result = (residual.astype(jnp.float32) + jnp.dot(activated, w_proj, preferred_element_type=jnp.float32)).astype(jnp.bfloat16)
    return result.reshape(GROUPS, WINDOW, D)
```

```python
import jax
import jax.numpy as jnp
from jax import lax
from jax.experimental import pallas as pl
from jax.experimental.pallas import tpu as pltpu
from jax.sharding import PartitionSpec as P

HEADS = 16
HEAD = 64
LANES = 128
KEY_CHUNK = 512
LOG2E = 1.4426950408889634

epsilon = 1e-05
big_negative = -1e30


VMEM = pl.BlockSpec(memory_space=pltpu.VMEM)
SMEM = pl.BlockSpec(memory_space=pltpu.SMEM)


def coords(index):
    b, g = divmod(index, 16)
    return g // 4, (g // 2) % 2, g % 2, b // 2, b % 2


def flat(x, yh, core, z, yl):
    return ((z % 8) * 2 + yl) * 16 + (x % 4) * 4 + yh * 2 + core


def send(value, target):
    pairs = []
    for source in range(256):
        to = target(*coords(source))
        if to is not None:
            pairs.append((source, to if isinstance(to, int) else flat(*to)))
    return lax.ppermute(value, ("blk", "grp"), pairs)


def normalize(values, row_gain):
    center = values - jnp.mean(values, axis=-1, keepdims=True)
    spread = jnp.mean(center * center, axis=-1, keepdims=True)
    return center * lax.rsqrt(spread + epsilon) * row_gain


def segment_of(utt_lengths, positions):
    starts = jnp.cumsum(utt_lengths) - utt_lengths
    started = (starts[None, :] <= positions[:, None]).astype(jnp.int32)
    return jnp.sum(started, axis=1) - 1


def low_lanes(rows):
    return lax.broadcasted_iota(jnp.int32, (rows, LANES), 1) < HEAD


def swap_lanes(values):
    return pltpu.roll(values, HEAD, 1)


def qkv_kernel(slot_ref, own_ref, other_ref, gain_ref, *refs):
    shards, (key_values, queries), (weights, normed) = refs[:8], (refs[8:16], refs[16:24]), refs[24:]
    rows = own_ref.shape[0]
    gain = gain_ref[0:1, :]
    normed[:rows] = normalize(own_ref[...].astype(jnp.float32), gain).astype(jnp.bfloat16)
    normed[rows:] = normalize(other_ref[...].astype(jnp.float32), gain).astype(jnp.bfloat16)
    for i in range(8):
        weights[slot_ref[i]] = shards[i][...]
    contract = (((1,), (1,)), ((), ()))
    low = low_lanes(rows)
    for d in range(8):
        both = lax.dot_general(
            normed[...], weights[d, HEAD:, :], contract, preferred_element_type=jnp.float32
        )
        key_values[d][...] = both.astype(jnp.bfloat16)
        query = lax.dot_general(
            normed[...], weights[d, :HEAD, :], contract, preferred_element_type=jnp.float32
        ) * (HEAD**-0.5 * LOG2E)
        queries[d][...] = jnp.concatenate([query[:rows], query[rows:]], axis=1).astype(jnp.bfloat16)


def project_qkv(slots, own, other, gain, shards):
    rows = own.shape[0]
    shapes = [jax.ShapeDtypeStruct((2 * rows, LANES), jnp.bfloat16)] * 8
    shapes += [jax.ShapeDtypeStruct((rows, LANES), jnp.bfloat16)] * 8
    return pl.pallas_call(
        qkv_kernel,
        out_shape=shapes,
        in_specs=[SMEM] + [VMEM] * 11,
        out_specs=[VMEM] * 16,
        scratch_shapes=[
            pltpu.VMEM((8,) + shards[0].shape, jnp.bfloat16),
            pltpu.VMEM((2 * rows, own.shape[1]), jnp.bfloat16),
        ],
        compiler_params=pltpu.CompilerParams(vmem_limit_bytes=40 * 1024 * 1024),
    )(slots, own, other, gain, *shards)


def attend_kernel(base_ref, lo_ref, hi_ref, *refs):
    chunk_q, chunk_kv, outs = refs[:8], refs[8:16], refs[16:32]
    keys, values, queries, scores_a, scores_b, max_a, max_b, mixed_all = refs[32:]
    half = chunk_q[0].shape[0]
    block = half
    window = keys.shape[0]
    blocks = window // block
    low = low_lanes(block)
    lo, hi = lo_ref[0:1, :], hi_ref[0:1, :]
    row = lax.broadcasted_iota(jnp.int32, (block, LANES), 0)
    for i in range(blocks):
        d, side = divmod(i, 2)
        position = row + base_ref[i]
        inside = (position >= lo) & (position < hi)
        part = chunk_kv[d][side * half : (side + 1) * half, :].astype(jnp.float32)
        at = slice(i * block, (i + 1) * block)
        keys[at] = jnp.where(low, part, jnp.where(inside, 0.0, big_negative)).astype(jnp.bfloat16)
        values[at] = jnp.where(low, 1.0, part).astype(jnp.bfloat16)
        query = chunk_q[d][...].astype(jnp.float32)
        query = swap_lanes(query) if side else query
        queries[at] = jnp.where(low, query, jnp.where(inside, 1.0, 0.0)).astype(jnp.bfloat16)
    chunks = window // KEY_CHUNK

    def score(query, j, scores, best):
        part = lax.dot_general(
            query,
            keys[j * KEY_CHUNK : (j + 1) * KEY_CHUNK, :],
            (((1,), (1,)), ((), ())),
            preferred_element_type=jnp.float32,
        )
        scores[:, j * KEY_CHUNK : (j + 1) * KEY_CHUNK] = part
        for t in range(KEY_CHUNK // LANES):
            piece = part[:, t * LANES : (t + 1) * LANES]
            best = piece if best is None else jnp.maximum(best, piece)
        return best

    def weigh(j, scores, row_max, total):
        probs = jnp.exp2(scores[:, j * KEY_CHUNK : (j + 1) * KEY_CHUNK] - row_max)
        part = jnp.dot(
            probs.astype(jnp.bfloat16),
            values[j * KEY_CHUNK : (j + 1) * KEY_CHUNK, :],
            preferred_element_type=jnp.float32,
        )
        return part if total is None else total + part

    def finish(total, i):
        mixed = total / swap_lanes(total)
        upper = swap_lanes(mixed[: block // 2])
        packed = jnp.where(low[: block // 2], upper, mixed[block // 2 :]).astype(jnp.bfloat16)
        mixed_all[pl.ds(pl.multiple_of(i * (block // 2), block // 2), block // 2), :] = packed

    def both(i, new, old, j_old):
        query = queries[pl.ds(pl.multiple_of(i * block, block), block), :]
        row_max = old[1][:, 0:1]
        best, total = None, None
        for j in range(chunks):
            best = score(query, j, new[0], best)
            total = weigh(j, old[0], row_max, total)
        new[1][...] = jnp.broadcast_to(jnp.max(best, axis=1, keepdims=True), (block, LANES))
        finish(total, j_old)

    buffer_a, buffer_b = (scores_a, max_a), (scores_b, max_b)

    def step(i, carry):
        both(2 * i, buffer_a, buffer_b, jnp.maximum(2 * i - 1, 0))
        both(2 * i + 1, buffer_b, buffer_a, 2 * i)
        return carry

    lax.fori_loop(0, blocks // 2, step, 0)
    total = None
    for j in range(chunks):
        total = weigh(j, scores_b, max_b[:, 0:1], total)
    finish(total, blocks - 1)
    for i in range(blocks):
        outs[i][...] = mixed_all[i * (block // 2) : (i + 1) * (block // 2), :]


def attend(bases, lo, hi, chunk_q, chunk_kv):
    half = chunk_q[0].shape[0]
    window = 16 * half
    return pl.pallas_call(
        attend_kernel,
        out_shape=[jax.ShapeDtypeStruct((half // 2, LANES), jnp.bfloat16)] * 16,
        in_specs=[SMEM] + [VMEM] * 18,
        out_specs=[VMEM] * 16,
        scratch_shapes=[pltpu.VMEM((window, LANES), jnp.bfloat16)] * 3
        + [pltpu.VMEM((half, window), jnp.float32)] * 2
        + [pltpu.VMEM((half, LANES), jnp.float32)] * 2
        + [pltpu.VMEM((window // 2, LANES), jnp.bfloat16)],
        compiler_params=pltpu.CompilerParams(vmem_limit_bytes=48 * 1024 * 1024),
    )(bases, lo, hi, *chunk_q, *chunk_kv)


def gate_kernel(where_ref, *refs):
    own, other = refs[:8], refs[8:16]
    frames, w_out, gain, w_glu, residual_ref, gated_ref = refs[16:]
    half = own[0].shape[0]
    low = low_lanes(half)
    first = where_ref[1] == 0
    total = frames[...].astype(jnp.float32)
    for d in range(8):
        mine, theirs = own[d][...].astype(jnp.float32), other[d][...].astype(jnp.float32)
        even, odd = jnp.where(first, mine, theirs), jnp.where(first, theirs, mine)
        upper = jnp.where(low, even, swap_lanes(odd))
        lower = jnp.where(low, swap_lanes(even), odd)
        attended = jnp.concatenate([upper, lower], axis=0).astype(jnp.bfloat16)
        at = lax.rem(where_ref[0] + d, 8) * LANES
        total = total + jnp.dot(
            attended, w_out[pl.ds(pl.multiple_of(at, LANES), LANES), :], preferred_element_type=jnp.float32
        )
    residual = total.astype(jnp.bfloat16)
    residual_ref[...] = residual
    width = frames.shape[1]
    conv_in = normalize(residual.astype(jnp.float32), gain[0:1, :]).astype(jnp.bfloat16)
    step = 256
    for j in range(0, width, step):
        a = jnp.dot(conv_in, w_glu[:, j : j + step], preferred_element_type=jnp.float32)
        b = jnp.dot(conv_in, w_glu[:, width + j : width + j + step], preferred_element_type=jnp.float32)
        gated_ref[:, j : j + step] = (a * jax.nn.sigmoid(b)).astype(jnp.bfloat16)


def gate(where, own, other, frames, w_out, gain, w_glu):
    shape = jax.ShapeDtypeStruct(frames.shape, jnp.bfloat16)
    return pl.pallas_call(
        gate_kernel,
        out_shape=[shape, shape],
        in_specs=[SMEM] + [VMEM] * 20,
        out_specs=[VMEM] * 2,
        compiler_params=pltpu.CompilerParams(vmem_limit_bytes=40 * 1024 * 1024),
    )(where, *own, *other, frames, w_out, gain, w_glu)


def body(
    frames, utt_lengths, attn_gain, w_qkv, w_out, conv_gain, w_glu, w_depth, depth_gain, w_proj
):
    frame_rows = frames.shape[1]
    width = frames.shape[2]
    kernel_half = (w_depth.shape[0] - 1) // 2
    block_index = lax.axis_index("blk")
    group_index = lax.axis_index("grp")
    z, yl = block_index // 2, block_index % 2
    x, core = group_index // 4, group_index % 2
    window_start = group_index * (16 * frame_rows)
    first_frame = window_start + block_index * frame_rows
    local_frames = frames[0]

    other_frames = send(local_frames, lambda x, yh, c, z, yl: (x, yh, c, z, 1 - yl))
    shard = w_qkv.T

    def route(offset):
        return lambda x, yh, c, z, yl: (
            (x - offset, yh, yh, z, c) if yl == c else (x - offset, 1 - yh, yh, z, c)
        )

    offsets = (0, 1, 3, 2)
    shards = [send(shard, route(offset)) for offset in offsets]
    shards += [send(s, lambda x, yh, c, z, yl: (x, yh, 1 - c, z, yl)) for s in shards]
    slots = [(2 * ((x + offset) % 4) + c) for c in (core, 1 - core) for offset in offsets]
    slots = jnp.stack([(s - z) % 8 for s in slots]).astype(jnp.int32)
    outs = project_qkv(slots, local_frames, other_frames, attn_gain[None, :], shards)
    own_kv, own_q = outs[:8], outs[8:]

    def along(d):
        return lambda x, yh, c, z, yl: (x, yh, c, z + d, yl)

    order = (4, 3, 5, 2, 6, 1, 7)
    chunk_kv, chunk_q = [own_kv[0]] + [None] * 7, [own_q[0]] + [None] * 7
    for d in order:
        chunk_kv[d] = send(own_kv[d], along(d))
    for d in order:
        chunk_q[d] = send(own_q[d], along(d))
    bases = jnp.stack(
        [
            window_start + (((z - d) % 8) * 2 + side) * frame_rows
            for d in range(8)
            for side in (yl, 1 - yl)
        ]
    ).astype(jnp.int32)
    ends = jnp.cumsum(utt_lengths)
    count = utt_lengths.shape[0]
    lo = jnp.zeros((1, LANES), jnp.int32).at[0, HEAD : HEAD + count].set(ends - utt_lengths)
    hi = jnp.zeros((1, LANES), jnp.int32).at[0, HEAD : HEAD + count].set(ends)
    mixed = attend(bases, lo, hi, chunk_q, chunk_kv)

    def back(d, cross):
        return lambda x, yh, c, z, yl: (x, yh, c, z - d, 1 - yl if cross else yl)

    own_out, other_out = [mixed[0]] + [None] * 7, [None] * 8
    for d in order:
        other_out[d] = send(mixed[2 * d + 1], back(d, True))
        own_out[d] = send(mixed[2 * d], back(d, False))
    other_out[0] = send(mixed[1], back(0, True))
    residual, gated = gate(
        jnp.stack([z, yl]).astype(jnp.int32),
        own_out,
        other_out,
        local_frames,
        w_out,
        conv_gain[None, :],
        w_glu,
    )

    def neighbour(step):
        def target(x, yh, c, z, yl):
            place = (x * 4 + yh * 2 + c) * 16 + z * 2 + yl + step
            return (place % 16) * 16 + place // 16 if 0 <= place < 256 else None

        return target

    rim = kernel_half + 1
    left = send(gated[frame_rows - rim :], neighbour(1))
    right = send(gated[:rim], neighbour(-1))
    local_seg = segment_of(utt_lengths, first_frame + jnp.arange(frame_rows, dtype=jnp.int32))
    extended = jnp.concatenate([left[1:], gated, right[:-1]], axis=0).astype(jnp.float32)
    extended_seg = segment_of(
        utt_lengths,
        first_frame - kernel_half + jnp.arange(frame_rows + 2 * kernel_half, dtype=jnp.int32),
    )
    mixed_conv = jnp.zeros((frame_rows, width), jnp.float32)
    for offset in range(2 * kernel_half + 1):
        same_seg = (extended_seg[offset : offset + frame_rows] == local_seg)[:, None]
        mixed_conv = mixed_conv + jnp.where(
            same_seg, extended[offset : offset + frame_rows] * w_depth[offset], 0.0
        )
    normed_conv = normalize(mixed_conv, depth_gain)
    activated = (normed_conv * jax.nn.sigmoid(normed_conv)).astype(jnp.bfloat16)
    result = (
        residual.astype(jnp.float32)
        + jnp.dot(activated, w_proj, preferred_element_type=jnp.float32)
    ).astype(jnp.bfloat16)
    return result[None]


def solution(mesh):
    in_specs = (P("grp", "blk", None), P(), P(), P(None, "grp"), P(), P(), P(), P(), P(), P())
    out_specs = P("grp", "blk", None)
    return jax.shard_map(body, mesh=mesh, in_specs=in_specs, out_specs=out_specs, check_vma=False)
```

```python
import jax
import jax.numpy as jnp
from jax import lax
from jax.experimental import pallas as pl
from jax.experimental.pallas import tpu as pltpu
from jax.sharding import PartitionSpec as P


HEAD = 64
LANES = 128
KEY_CHUNK = 512
QUERY_PARTS = 2
OFFSETS = (0, 1, 3, 2)
LOG2E = 1.4426950408889634

epsilon = 1e-05
big_negative = -1e30


VMEM = pl.BlockSpec(memory_space=pltpu.VMEM)
SMEM = pl.BlockSpec(memory_space=pltpu.SMEM)


def coords(index):
    b, g = divmod(index, 16)
    return g // 4, (g // 2) % 2, g % 2, b // 2, b % 2


def flat(x, yh, core, z, yl):
    return ((z % 8) * 2 + yl) * 16 + (x % 4) * 4 + yh * 2 + core


def send(value, target):
    pairs = []
    for source in range(256):
        to = target(*coords(source))
        if to is not None:
            pairs.append((source, to if isinstance(to, int) else flat(*to)))
    return lax.ppermute(value, ("blk", "grp"), pairs)


def normalize(values, row_gain):
    center = values - jnp.mean(values, axis=-1, keepdims=True)
    spread = jnp.mean(center * center, axis=-1, keepdims=True)
    return center * lax.rsqrt(spread + epsilon) * row_gain


def segment_of(utt_lengths, positions):
    starts = jnp.cumsum(utt_lengths) - utt_lengths
    started = (starts[None, :] <= positions[:, None]).astype(jnp.int32)
    return jnp.sum(started, axis=1) - 1


def low_lanes(rows):
    return lax.broadcasted_iota(jnp.int32, (rows, LANES), 1) < HEAD


def swap_lanes(values):
    return pltpu.roll(values, HEAD, 1)


def project(normed, slot_ref, shards, weights, scale):
    near, far = shards[:4], shards[4]
    for i in range(4):
        weights[pl.ds(pl.multiple_of(slot_ref[i] * HEAD, HEAD), HEAD), :] = near[i][...]
        weights[pl.ds(pl.multiple_of(slot_ref[4 + i] * HEAD, HEAD), HEAD), :] = far[i * HEAD : (i + 1) * HEAD]
    rows = normed.shape[0] // 2
    low = low_lanes(rows)
    for pair in range(4):
        both = lax.dot_general(
            normed[...],
            weights[pair * LANES : (pair + 1) * LANES, :],
            (((1,), (1,)), ((), ())),
            preferred_element_type=jnp.float32,
        )
        if scale is not None:
            both = both * scale
        own, other = both[:rows], both[rows:]
        yield 2 * pair, jnp.where(low, own, swap_lanes(other)).astype(jnp.bfloat16)
        yield 2 * pair + 1, jnp.where(low, swap_lanes(own), other).astype(jnp.bfloat16)


def first_kernel(slot_ref, own_ref, other_ref, gain_ref, *refs):
    shards, (out, normed), weights = refs[:5], refs[5:7], refs[7]
    rows = own_ref.shape[0]
    gain = gain_ref[0:1, :]
    normed[:rows] = normalize(own_ref[...].astype(jnp.float32), gain).astype(jnp.bfloat16)
    normed[rows:] = normalize(other_ref[...].astype(jnp.float32), gain).astype(jnp.bfloat16)
    for head, packed in project(normed, slot_ref, shards, weights, None):
        out[head] = packed


def project_first(slots, own, other, gain, shards):
    rows, width = own.shape
    return pl.pallas_call(
        first_kernel,
        out_shape=[
            jax.ShapeDtypeStruct((8, rows, LANES), jnp.bfloat16),
            jax.ShapeDtypeStruct((2 * rows, width), jnp.bfloat16),
        ],
        in_specs=[SMEM] + [VMEM] * 8,
        out_specs=[VMEM] * 2,
        scratch_shapes=[pltpu.VMEM((8 * HEAD, width), jnp.bfloat16)],
        compiler_params=pltpu.CompilerParams(vmem_limit_bytes=24 * 1024 * 1024),
    )(slots, own, other, gain, *shards)


def next_kernel(parts, scale):
    def kernel(slot_ref, normed, *refs):
        shards, outs, weights = refs[:5], refs[5:-1], refs[-1]
        step = outs[0].shape[1]
        for head, packed in project(normed, slot_ref, shards, weights, scale):
            for i in range(parts):
                outs[i][head] = packed[i * step : (i + 1) * step]

    return kernel


def project_next(slots, normed, shards, parts, scale):
    rows, width = normed.shape[0] // 2, normed.shape[1]
    return pl.pallas_call(
        next_kernel(parts, scale),
        out_shape=[jax.ShapeDtypeStruct((8, rows // parts, LANES), jnp.bfloat16)] * parts,
        in_specs=[SMEM] + [VMEM] * 6,
        out_specs=[VMEM] * parts,
        scratch_shapes=[pltpu.VMEM((8 * HEAD, width), jnp.bfloat16)],
        compiler_params=pltpu.CompilerParams(vmem_limit_bytes=24 * 1024 * 1024),
    )(slots, normed, *shards)


def attend_kernel(base_ref, lo_ref, hi_ref, q_ref, k_ref, v_ref, out_ref, *scratch):
    keys, values, queries, scores_a, scores_b, max_a, max_b = scratch
    sources, half, _ = k_ref.shape
    part = q_ref.shape[1]
    block = 2 * part
    lo, hi = lo_ref[0:1, :], hi_ref[0:1, :]

    def inside(rows, base):
        position = lax.broadcasted_iota(jnp.int32, (rows, LANES), 0) + base
        return (position >= lo) & (position < hi)

    low_half, low_part, low_quarter = low_lanes(half), low_lanes(part), low_lanes(part // 2)

    def prepare(s, carry):
        key, value, query = (ref[s].astype(jnp.float32) for ref in (k_ref, v_ref, q_ref))
        for side in range(2):
            base = base_ref[side] + s * (2 * half)
            at = pl.ds(pl.multiple_of(s * (2 * half) + side * half, half), half)
            mask = jnp.where(inside(half, base), 0.0, big_negative)
            keys[at, :] = jnp.where(low_half, swap_lanes(key) if side else key, mask).astype(jnp.bfloat16)
            values[at, :] = jnp.where(low_half, 1.0, value if side else swap_lanes(value)).astype(jnp.bfloat16)
            at = pl.ds(pl.multiple_of(s * block + side * part, part), part)
            mark = jnp.where(inside(part, base + base_ref[2]), 1.0, 0.0)
            queries[at, :] = jnp.where(low_part, swap_lanes(query) if side else query, mark).astype(jnp.bfloat16)
        return carry

    lax.fori_loop(0, sources, prepare, 0)
    window = keys.shape[0]
    chunks = window // KEY_CHUNK

    def score(query, j, scores, best):
        part = lax.dot_general(
            query,
            keys[j * KEY_CHUNK : (j + 1) * KEY_CHUNK, :],
            (((1,), (1,)), ((), ())),
            preferred_element_type=jnp.float32,
        )
        scores[:, j * KEY_CHUNK : (j + 1) * KEY_CHUNK] = part
        for t in range(KEY_CHUNK // LANES):
            piece = part[:, t * LANES : (t + 1) * LANES]
            best = piece if best is None else jnp.maximum(best, piece)
        return best

    def weigh(j, scores, row_max, total):
        probs = jnp.exp2(scores[:, j * KEY_CHUNK : (j + 1) * KEY_CHUNK] - row_max)
        part = jnp.dot(
            probs.astype(jnp.bfloat16),
            values[j * KEY_CHUNK : (j + 1) * KEY_CHUNK, :],
            preferred_element_type=jnp.float32,
        )
        return part if total is None else total + part

    def finish(total, source):
        mixed = total / swap_lanes(total)
        for side in range(2):
            upper = swap_lanes(mixed[side * part : side * part + part // 2])
            lower = mixed[side * part + part // 2 : (side + 1) * part]
            out_ref[2 * source + base_ref[3 + side]] = jnp.where(low_quarter, upper, lower).astype(jnp.bfloat16)

    def both(i, new, old, i_old):
        query = queries[pl.ds(pl.multiple_of(i * block, block), block), :]
        row_max = old[1][:, 0:1]
        best, total = None, None
        for j in range(chunks):
            best = score(query, j, new[0], best)
            total = weigh(j, old[0], row_max, total)
        new[1][...] = jnp.broadcast_to(jnp.max(best, axis=1, keepdims=True), (block, LANES))
        finish(total, i_old)

    buffer_a, buffer_b = (scores_a, max_a), (scores_b, max_b)

    def step(i, carry):
        both(2 * i, buffer_a, buffer_b, jnp.maximum(2 * i - 1, 0))
        both(2 * i + 1, buffer_b, buffer_a, 2 * i)
        return carry

    lax.fori_loop(0, sources // 2, step, 0)
    total = None
    for j in range(chunks):
        total = weigh(j, scores_b, max_b[:, 0:1], total)
    finish(total, sources - 1)


def attend(bases, lo, hi, query, key, value):
    sources, half, _ = key.shape
    part = query.shape[1]
    window = 2 * half * sources
    return pl.pallas_call(
        attend_kernel,
        out_shape=jax.ShapeDtypeStruct((2 * sources, part // 2, LANES), jnp.bfloat16),
        in_specs=[SMEM] + [VMEM] * 5,
        out_specs=VMEM,
        scratch_shapes=[pltpu.VMEM((window, LANES), jnp.bfloat16)] * 2
        + [pltpu.VMEM((2 * part * sources, LANES), jnp.bfloat16)]
        + [pltpu.VMEM((2 * part, window), jnp.float32)] * 2
        + [pltpu.VMEM((2 * part, LANES), jnp.float32)] * 2,
        compiler_params=pltpu.CompilerParams(vmem_limit_bytes=24 * 1024 * 1024),
    )(bases, lo, hi, query, key, value)


def gate_kernel(*refs):
    parts = refs[:QUERY_PARTS]
    frames, gain, w_out_hbm, w_glu_hbm, residual_ref, gated_ref = refs[QUERY_PARTS:-5]
    w_out, w_glu, attended, out_sem, glu_sem = refs[-5:]
    out_copy = pltpu.make_async_copy(w_out_hbm, w_out, out_sem)
    glu_copy = pltpu.make_async_copy(w_glu_hbm, w_glu, glu_sem)
    out_copy.start()
    glu_copy.start()
    heads, quarter, _ = parts[0].shape
    low = low_lanes(quarter)
    for i in range(QUERY_PARTS):
        for pair in range(heads // 2):
            even = parts[i][2 * pair].astype(jnp.float32)
            odd = parts[i][2 * pair + 1].astype(jnp.float32)
            upper = jnp.where(low, even, swap_lanes(odd)).astype(jnp.bfloat16)
            lower = jnp.where(low, swap_lanes(even), odd).astype(jnp.bfloat16)
            at = slice(pair * LANES, (pair + 1) * LANES)
            attended[2 * i * quarter : (2 * i + 1) * quarter, at] = upper
            attended[(2 * i + 1) * quarter : (2 * i + 2) * quarter, at] = lower
    out_copy.wait()
    projected = jnp.dot(attended[...], w_out[...], preferred_element_type=jnp.float32)
    residual = (frames[...].astype(jnp.float32) + projected).astype(jnp.bfloat16)
    residual_ref[...] = residual
    width = frames.shape[1]
    conv_in = normalize(residual.astype(jnp.float32), gain[0:1, :]).astype(jnp.bfloat16)
    glu_copy.wait()
    step = 256
    for j in range(0, width, step):
        a = jnp.dot(conv_in, w_glu[:, j : j + step], preferred_element_type=jnp.float32)
        b = jnp.dot(conv_in, w_glu[:, width + j : width + j + step], preferred_element_type=jnp.float32)
        gated_ref[:, j : j + step] = (a * jax.nn.sigmoid(b)).astype(jnp.bfloat16)


def gate(parts, frames, gain, w_out, w_glu):
    shape = jax.ShapeDtypeStruct(frames.shape, jnp.bfloat16)
    anywhere = pl.BlockSpec(memory_space=pl.ANY)
    return pl.pallas_call(
        gate_kernel,
        out_shape=[shape, shape],
        in_specs=[VMEM] * (QUERY_PARTS + 2) + [anywhere] * 2,
        out_specs=[VMEM] * 2,
        scratch_shapes=[
            pltpu.VMEM(w_out.shape, jnp.bfloat16),
            pltpu.VMEM(w_glu.shape, jnp.bfloat16),
            pltpu.VMEM(frames.shape, jnp.bfloat16),
            pltpu.SemaphoreType.DMA,
            pltpu.SemaphoreType.DMA,
        ],
        compiler_params=pltpu.CompilerParams(vmem_limit_bytes=24 * 1024 * 1024),
    )(*parts, frames, gain, w_out, w_glu)


def body(
    frames, utt_lengths, attn_gain, w_qkv, w_out, conv_gain, w_glu, w_depth, depth_gain, w_proj
):
    frame_rows = frames.shape[1]
    width = frames.shape[2]
    kernel_half = (w_depth.shape[0] - 1) // 2
    block_index = lax.axis_index("blk")
    group_index = lax.axis_index("grp")
    yl = block_index % 2
    x, core = group_index // 4, group_index % 2
    window_start = group_index * (16 * frame_rows)
    first_frame = window_start + block_index * frame_rows
    local_frames = frames[0]

    other_frames = send(local_frames, lambda x, yh, c, z, yl: (x, yh, c, z, 1 - yl))
    shard = w_qkv.T

    def route(offset):
        return lambda x, yh, c, z, yl: (
            (x - offset, yh, yh, z, c) if yl == c else (x - offset, 1 - yh, yh, z, c)
        )

    def collect(part):
        own = shard[part * HEAD : (part + 1) * HEAD]
        near = [send(own, route(offset)) for offset in OFFSETS]
        swap = lambda x, yh, c, z, yl: (x, yh, 1 - c, z, yl)
        far = send(jnp.concatenate(near, axis=0), swap)
        return near + [far]

    slots = jnp.stack([2 * ((x + offset) % 4) + c for c in (core, 1 - core) for offset in OFFSETS])
    key_shards, value_shards, query_shards = collect(1), collect(2), collect(0)
    key, normed = project_first(slots, local_frames, other_frames, attn_gain[None, :], key_shards)
    (value,) = project_next(slots, normed, value_shards, 1, None)
    queries = project_next(slots, normed, query_shards, QUERY_PARTS, HEAD**-0.5 * LOG2E)

    def along_z(packed):
        groups = [[2 * z + yl for z in range(8)] for yl in range(2)]
        return lax.all_to_all(packed, "blk", 0, 0, axis_index_groups=groups, tiled=True)

    key, value = along_z(key), along_z(value)
    queries = [along_z(queries[i]) for i in range(QUERY_PARTS)]
    ends = jnp.cumsum(utt_lengths)
    pad = (HEAD, HEAD - utt_lengths.shape[0])
    lo = jnp.pad(ends - utt_lengths, pad)[None, :]
    hi = jnp.pad(ends, pad)[None, :]
    mixed = []
    for i in range(QUERY_PARTS):
        base = window_start + jnp.stack([yl, 1 - yl]) * frame_rows
        bases = jnp.concatenate([base, jnp.stack([i * (frame_rows // QUERY_PARTS) + 0 * yl, yl, 1 - yl])])
        part = attend(bases.astype(jnp.int32), lo, hi, queries[i], key, value)
        mixed.append(lax.all_to_all(part, "blk", 0, 0, tiled=True))
    residual, gated = gate(mixed, local_frames, conv_gain[None, :], w_out, w_glu)

    def neighbour(step):
        def target(x, yh, c, z, yl):
            place = (x * 4 + yh * 2 + c) * 16 + z * 2 + yl + step
            return (place % 16) * 16 + place // 16 if 0 <= place < 256 else None

        return target

    rim = kernel_half + 1
    left = send(gated[frame_rows - rim :], neighbour(1))
    right = send(gated[:rim], neighbour(-1))
    local_seg = segment_of(utt_lengths, first_frame + jnp.arange(frame_rows, dtype=jnp.int32))
    extended = jnp.concatenate([left[1:], gated, right[:-1]], axis=0).astype(jnp.float32)
    extended_seg = segment_of(
        utt_lengths,
        first_frame - kernel_half + jnp.arange(frame_rows + 2 * kernel_half, dtype=jnp.int32),
    )
    mixed_conv = jnp.zeros((frame_rows, width), jnp.float32)
    for offset in range(2 * kernel_half + 1):
        same_seg = (extended_seg[offset : offset + frame_rows] == local_seg)[:, None]
        mixed_conv = mixed_conv + jnp.where(
            same_seg, extended[offset : offset + frame_rows] * w_depth[offset], 0.0
        )
    normed_conv = normalize(mixed_conv, depth_gain)
    activated = (normed_conv * jax.nn.sigmoid(normed_conv)).astype(jnp.bfloat16)
    result = (
        residual.astype(jnp.float32)
        + jnp.dot(activated, w_proj, preferred_element_type=jnp.float32)
    ).astype(jnp.bfloat16)
    return result[None]


def solution(mesh):
    in_specs = (P("grp", "blk", None), P(), P(), P(None, "grp"), P(), P(), P(), P(), P(), P())
    out_specs = P("grp", "blk", None)
    return jax.shard_map(body, mesh=mesh, in_specs=in_specs, out_specs=out_specs, check_vma=False)
```

```python
import jax
import jax.numpy as jnp
from jax import lax
from jax.experimental import pallas as pl
from jax.experimental.pallas import tpu as pltpu
from jax.sharding import PartitionSpec as P


HEAD = 64
LANES = 128
KEY_CHUNK = 512
RIM = 16
ROWS = 16
OFFSETS = (0, 1, 3, 2)
LOG2E = 1.4426950408889634

epsilon = 1e-05
big_negative = -1e30


VMEM = pl.BlockSpec(memory_space=pltpu.VMEM)
SMEM = pl.BlockSpec(memory_space=pltpu.SMEM)
HBM = pl.BlockSpec(memory_space=pltpu.HBM)


def coords(index):
    b, g = divmod(index, 16)
    return g // 4, (g // 2) % 2, g % 2, b // 2, b % 2


def flat(x, yh, core, z, yl):
    return ((z % 8) * 2 + yl) * 16 + (x % 4) * 4 + yh * 2 + core


def send(value, target):
    pairs = []
    for source in range(256):
        to = target(*coords(source))
        if to is not None:
            pairs.append((source, to if isinstance(to, int) else flat(*to)))
    return lax.ppermute(value, ("blk", "grp"), pairs)


def normalize(values, row_gain):
    center = values - jnp.mean(values, axis=-1, keepdims=True)
    spread = jnp.mean(center * center, axis=-1, keepdims=True)
    return center * lax.rsqrt(spread + epsilon) * row_gain


def low_lanes(rows):
    return lax.broadcasted_iota(jnp.int32, (rows, LANES), 1) < HEAD


def swap_lanes(values):
    return pltpu.roll(values, HEAD, 1)


def project_kernel(slot_ref, own_ref, other_ref, gain_ref, *refs):
    shards, out, weights, normed, sems = refs[:8], refs[8], refs[9], refs[10], refs[11]
    copies = []
    for i, shard in enumerate(shards):
        at = pl.ds(pl.multiple_of(slot_ref[i] * HEAD, HEAD), HEAD)
        for j in range(3):
            copies.append(
                pltpu.make_async_copy(
                    shard.at[pl.ds(j * HEAD, HEAD)], weights.at[(j + 2) % 3, at], sems.at[3 * i + j]
                )
            )
            copies[-1].start()
    rows = own_ref.shape[0]
    gain = gain_ref[0:1, :]
    normed[:rows] = normalize(own_ref[...].astype(jnp.float32), gain).astype(jnp.bfloat16)
    normed[rows:] = normalize(other_ref[...].astype(jnp.float32), gain).astype(jnp.bfloat16)
    for copy in copies:
        copy.wait()
    low = low_lanes(rows)
    for part in range(3):
        at = slice(part * rows, (part + 1) * rows)
        for pair in range(4):
            both = lax.dot_general(
                normed[...],
                weights[part, pair * LANES : (pair + 1) * LANES, :],
                (((1,), (1,)), ((), ())),
                preferred_element_type=jnp.float32,
            )
            if part == 2:
                both = both * (HEAD**-0.5 * LOG2E)
            own, other = both[:rows], both[rows:]
            out[2 * pair, at] = jnp.where(low, own, swap_lanes(other)).astype(jnp.bfloat16)
            out[2 * pair + 1, at] = jnp.where(low, swap_lanes(own), other).astype(jnp.bfloat16)


def project_qkv(slots, own, other, gain, shards):
    rows, width = own.shape
    return pl.pallas_call(
        project_kernel,
        out_shape=jax.ShapeDtypeStruct((8, 3 * rows, LANES), jnp.bfloat16),
        in_specs=[SMEM] + [VMEM] * 3 + [HBM] * 8,
        out_specs=VMEM,
        scratch_shapes=[
            pltpu.VMEM((3, 8 * HEAD, width), jnp.bfloat16),
            pltpu.VMEM((2 * rows, width), jnp.bfloat16),
            pltpu.SemaphoreType.DMA((24,)),
        ],
        compiler_params=pltpu.CompilerParams(vmem_limit_bytes=24 * 1024 * 1024),
    )(slots, own, other, gain, *shards)


def attend_kernel(base_ref, lo_ref, hi_ref, in_ref, out_ref, *scratch):
    keys, values, queries, scores_a, scores_b, max_a, max_b = scratch
    sources = in_ref.shape[0]
    block = in_ref.shape[1] // 3
    lo, hi = lo_ref[0:1, :], hi_ref[0:1, :]
    low = low_lanes(block)
    row = lax.broadcasted_iota(jnp.int32, (block, LANES), 0)

    def prepare(s, carry):
        key, value, query = (
            in_ref[s, i * block : (i + 1) * block].astype(jnp.float32) for i in range(3)
        )
        for side in range(2):
            position = row + (base_ref[side] + s * (2 * block))
            inside = (position >= lo) & (position < hi)
            at = pl.ds(pl.multiple_of((2 * s + side) * block, block), block)
            mask, mark = jnp.where(inside, 0.0, big_negative), jnp.where(inside, 1.0, 0.0)
            keys[at, :] = jnp.where(low, swap_lanes(key) if side else key, mask).astype(jnp.bfloat16)
            values[at, :] = jnp.where(low, 1.0, value if side else swap_lanes(value)).astype(jnp.bfloat16)
            queries[at, :] = jnp.where(low, swap_lanes(query) if side else query, mark).astype(jnp.bfloat16)
        return carry

    lax.fori_loop(0, sources, prepare, 0)
    window = keys.shape[0]
    chunks = window // KEY_CHUNK

    def score(query, j, scores, best):
        part = lax.dot_general(
            query,
            keys[j * KEY_CHUNK : (j + 1) * KEY_CHUNK, :],
            (((1,), (1,)), ((), ())),
            preferred_element_type=jnp.float32,
        )
        scores[:, j * KEY_CHUNK : (j + 1) * KEY_CHUNK] = part
        for t in range(KEY_CHUNK // LANES):
            piece = part[:, t * LANES : (t + 1) * LANES]
            best = piece if best is None else jnp.maximum(best, piece)
        return best

    def weigh(j, scores, row_max, total):
        probs = jnp.exp2(scores[:, j * KEY_CHUNK : (j + 1) * KEY_CHUNK] - row_max)
        part = jnp.dot(
            probs.astype(jnp.bfloat16),
            values[j * KEY_CHUNK : (j + 1) * KEY_CHUNK, :],
            preferred_element_type=jnp.float32,
        )
        return part if total is None else total + part

    half = block // 2

    def finish(total, source, side):
        mixed = total / swap_lanes(total)
        packed = jnp.where(low[:half], swap_lanes(mixed[:half]), mixed[half:])
        out_ref[2 * source + base_ref[2 + side]] = packed.astype(jnp.bfloat16)

    def both(i, new, old, source_old, side_old):
        query = queries[pl.ds(pl.multiple_of(i * block, block), block), :]
        row_max = old[1][:, 0:1]
        best, total = None, None
        for j in range(chunks):
            best = score(query, j, new[0], best)
            total = weigh(j, old[0], row_max, total)
        new[1][...] = jnp.broadcast_to(jnp.max(best, axis=1, keepdims=True), (block, LANES))
        finish(total, source_old, side_old)

    buffer_a, buffer_b = (scores_a, max_a), (scores_b, max_b)

    def step(i, carry):
        both(2 * i, buffer_a, buffer_b, jnp.maximum(i - 1, 0), 1)
        both(2 * i + 1, buffer_b, buffer_a, i, 0)
        return carry

    lax.fori_loop(0, sources, step, 0)
    total = None
    for j in range(chunks):
        total = weigh(j, scores_b, max_b[:, 0:1], total)
    finish(total, sources - 1, 1)


def attend(bases, lo, hi, parts):
    sources, block = parts.shape[0], parts.shape[1] // 3
    window = 2 * block * sources
    return pl.pallas_call(
        attend_kernel,
        out_shape=jax.ShapeDtypeStruct((2 * sources, block // 2, LANES), jnp.bfloat16),
        in_specs=[SMEM] + [VMEM] * 3,
        out_specs=VMEM,
        scratch_shapes=[pltpu.VMEM((window, LANES), jnp.bfloat16)] * 3
        + [pltpu.VMEM((block, window), jnp.float32)] * 2
        + [pltpu.VMEM((block, LANES), jnp.float32)] * 2,
        compiler_params=pltpu.CompilerParams(vmem_limit_bytes=24 * 1024 * 1024),
    )(bases, lo, hi, parts)


def gate_kernel(mixed, frames, gain, w_out_hbm, w_glu_hbm, residual_ref, gated_ref, *scratch):
    w_out, w_glu, attended, out_sem, glu_sem = scratch
    out_copy = pltpu.make_async_copy(w_out_hbm, w_out, out_sem)
    glu_copy = pltpu.make_async_copy(w_glu_hbm, w_glu, glu_sem)
    out_copy.start()
    glu_copy.start()
    heads, half, _ = mixed.shape
    low = low_lanes(half)
    for pair in range(heads // 2):
        even, odd = mixed[2 * pair].astype(jnp.float32), mixed[2 * pair + 1].astype(jnp.float32)
        at = slice(pair * LANES, (pair + 1) * LANES)
        attended[:half, at] = jnp.where(low, even, swap_lanes(odd)).astype(jnp.bfloat16)
        attended[half:, at] = jnp.where(low, swap_lanes(even), odd).astype(jnp.bfloat16)
    out_copy.wait()
    projected = jnp.dot(attended[...], w_out[...], preferred_element_type=jnp.float32)
    residual = (frames[...].astype(jnp.float32) + projected).astype(jnp.bfloat16)
    residual_ref[...] = residual
    width = frames.shape[1]
    conv_in = normalize(residual.astype(jnp.float32), gain[0:1, :]).astype(jnp.bfloat16)
    glu_copy.wait()
    step = 256
    for j in range(0, width, step):
        a = jnp.dot(conv_in, w_glu[:, j : j + step], preferred_element_type=jnp.float32)
        b = jnp.dot(conv_in, w_glu[:, width + j : width + j + step], preferred_element_type=jnp.float32)
        gated_ref[:, j : j + step] = (a * jax.nn.sigmoid(b)).astype(jnp.bfloat16)


def gate(mixed, frames, gain, w_out, w_glu):
    shape = jax.ShapeDtypeStruct(frames.shape, jnp.bfloat16)
    return pl.pallas_call(
        gate_kernel,
        out_shape=[shape, shape],
        in_specs=[VMEM] * 3 + [HBM] * 2,
        out_specs=[VMEM] * 2,
        scratch_shapes=[
            pltpu.VMEM(w_out.shape, jnp.bfloat16),
            pltpu.VMEM(w_glu.shape, jnp.bfloat16),
            pltpu.VMEM(frames.shape, jnp.bfloat16),
            pltpu.SemaphoreType.DMA,
            pltpu.SemaphoreType.DMA,
        ],
        compiler_params=pltpu.CompilerParams(vmem_limit_bytes=24 * 1024 * 1024),
    )(mixed, frames, gain, w_out, w_glu)


def convolve(source, row, weights, t_first, t_last, position, start_ref, end_ref, masked):
    place = lax.broadcasted_iota(jnp.int32, (ROWS, LANES), 0) + position
    lo, hi = jnp.zeros_like(place), jnp.zeros_like(place)
    if masked:
        for u in range(start_ref.shape[0]):
            inside = (place >= start_ref[u]) & (place < end_ref[u])
            lo, hi = jnp.where(inside, start_ref[u], lo), jnp.where(inside, end_ref[u], hi)
        lo, hi = lo - place, hi - place
    tiles = source.shape[0]
    totals = [None] * tiles
    for t in range(t_first, t_last):
        same = (lo <= t - RIM + 1) & (hi > t - RIM + 1) if masked else None
        for c in range(tiles):
            term = source[c, pl.ds(row + t + 1, ROWS), :] * weights[t : t + 1, c * LANES : (c + 1) * LANES]
            term = jnp.where(same, term, 0.0) if masked else term
            totals[c] = term if totals[c] is None else totals[c] + term
    return totals


def inner_kernel(first_ref, start_ref, end_ref, gated, weights, out, padded):
    rows, width = gated.shape
    for c in range(width // LANES):
        padded[c, :RIM] = jnp.zeros((RIM, LANES), jnp.float32)
        padded[c, RIM : RIM + rows] = gated[:, c * LANES : (c + 1) * LANES].astype(jnp.float32)
        padded[c, RIM + rows :] = jnp.zeros((RIM, LANES), jnp.float32)

    def step(i, carry):
        row = pl.multiple_of(i * ROWS, ROWS)
        position = first_ref[0] + row
        crossed = False
        for u in range(1, start_ref.shape[0]):
            crossed |= (start_ref[u] > position - RIM) & (start_ref[u] < position + ROWS + RIM)

        def run(masked):
            totals = convolve(
                padded, row, weights, 0, weights.shape[0], position, start_ref, end_ref, masked
            )
            for c, total in enumerate(totals):
                out[pl.ds(row, ROWS), c * LANES : (c + 1) * LANES] = total

        pl.when(crossed)(lambda: run(True))
        pl.when(jnp.logical_not(crossed))(lambda: run(False))
        return carry

    lax.fori_loop(0, rows // ROWS, step, 0)


def convolve_inner(first, starts, ends, gated, weights):
    rows, width = gated.shape
    return pl.pallas_call(
        inner_kernel,
        out_shape=jax.ShapeDtypeStruct(gated.shape, jnp.float32),
        in_specs=[SMEM] * 3 + [VMEM] * 2,
        out_specs=VMEM,
        scratch_shapes=[pltpu.VMEM((width // LANES, rows + 2 * RIM, LANES), jnp.float32)],
        compiler_params=pltpu.CompilerParams(vmem_limit_bytes=16 * 1024 * 1024),
    )(first, starts, ends, gated, weights)


def last_kernel(
    first_ref, start_ref, end_ref, inner, left, right, residual, weights, gain, w_proj_hbm, out, *scratch
):
    w_proj, total, edge, sem = scratch
    copy = pltpu.make_async_copy(w_proj_hbm, w_proj, sem)
    copy.start()
    rows, width = inner.shape
    total[...] = inner[...]
    count = weights.shape[0]
    for side, rim in enumerate((left, right)):
        at = 0 if side == 0 else 2 * RIM
        row = 0 if side == 0 else rows - ROWS
        for c in range(width // LANES):
            edge[c] = jnp.zeros(edge.shape[1:], jnp.float32)
            edge[c, at : at + RIM] = rim[:, c * LANES : (c + 1) * LANES].astype(jnp.float32)
        span = (0, RIM - 1) if side == 0 else (RIM, count)
        parts = convolve(
            edge, 0, weights, *span, first_ref[0] + row, start_ref, end_ref, True
        )
        for c, part in enumerate(parts):
            lanes = slice(c * LANES, (c + 1) * LANES)
            total[row : row + ROWS, lanes] = total[row : row + ROWS, lanes] + part
    normed = normalize(total[...], gain[0:1, :])
    activated = (normed * jax.nn.sigmoid(normed)).astype(jnp.bfloat16)
    copy.wait()
    projected = jnp.dot(activated, w_proj[...], preferred_element_type=jnp.float32)
    out[...] = (residual[...].astype(jnp.float32) + projected).astype(jnp.bfloat16)


def finish_block(first, starts, ends, inner, left, right, residual, weights, gain, w_proj):
    _, width = inner.shape
    return pl.pallas_call(
        last_kernel,
        out_shape=jax.ShapeDtypeStruct(residual.shape, jnp.bfloat16),
        in_specs=[SMEM] * 3 + [VMEM] * 6 + [HBM],
        out_specs=VMEM,
        scratch_shapes=[
            pltpu.VMEM(w_proj.shape, jnp.bfloat16),
            pltpu.VMEM(inner.shape, jnp.float32),
            pltpu.VMEM((width // LANES, 3 * RIM, LANES), jnp.float32),
            pltpu.SemaphoreType.DMA,
        ],
        compiler_params=pltpu.CompilerParams(vmem_limit_bytes=24 * 1024 * 1024),
    )(first, starts, ends, inner, left, right, residual, weights, gain, w_proj)


def body(
    frames, utt_lengths, attn_gain, w_qkv, w_out, conv_gain, w_glu, w_depth, depth_gain, w_proj
):
    frame_rows = frames.shape[1]
    block_index = lax.axis_index("blk")
    group_index = lax.axis_index("grp")
    yl = block_index % 2
    x, core = group_index // 4, group_index % 2
    window_start = group_index * (16 * frame_rows)
    first_frame = window_start + block_index * frame_rows
    local_frames = frames[0]

    other_frames = send(local_frames, lambda x, yh, c, z, yl: (x, yh, c, z, 1 - yl))
    shard = w_qkv.T

    def route(offset):
        return lambda x, yh, c, z, yl: (
            (x - offset, yh, yh, z, c) if yl == c else (x - offset, 1 - yh, yh, z, c)
        )

    near = [send(shard, route(offset)) for offset in OFFSETS]
    swap = lambda x, yh, c, z, yl: (x, yh, 1 - c, z, yl)
    far = [send(piece, swap) for piece in near]
    slots = jnp.stack([2 * ((x + offset) % 4) + c for c in (core, 1 - core) for offset in OFFSETS])
    parts = project_qkv(slots, local_frames, other_frames, attn_gain[None, :], near + far)
    groups = [[2 * z + yl for z in range(8)] for yl in range(2)]
    parts = lax.all_to_all(parts, "blk", 0, 0, axis_index_groups=groups, tiled=True)
    ends = jnp.cumsum(utt_lengths)
    starts = ends - utt_lengths
    pad = (HEAD, HEAD - utt_lengths.shape[0])
    sides = jnp.stack([yl, 1 - yl])
    bases = jnp.concatenate([window_start + sides * frame_rows, sides])
    mixed = attend(bases, jnp.pad(starts, pad)[None, :], jnp.pad(ends, pad)[None, :], parts)
    mixed = lax.all_to_all(mixed, "blk", 0, 0, tiled=True)
    residual, gated = gate(mixed, local_frames, conv_gain[None, :], w_out, w_glu)

    def neighbour(step):
        def target(x, yh, c, z, yl):
            place = (x * 4 + yh * 2 + c) * 16 + z * 2 + yl + step
            return (place % 16) * 16 + place // 16 if 0 <= place < 256 else None

        return target

    left = send(gated[frame_rows - RIM :], neighbour(1))
    right = send(gated[:RIM], neighbour(-1))
    where = (first_frame[None], starts, ends)
    inner = convolve_inner(*where, gated, w_depth)
    result = finish_block(*where, inner, left, right, residual, w_depth, depth_gain[None, :], w_proj)
    return result[None]


def solution(mesh):
    in_specs = (P("grp", "blk", None), P(), P(), P(None, "grp"), P(), P(), P(), P(), P(), P())
    out_specs = P("grp", "blk", None)
    return jax.shard_map(body, mesh=mesh, in_specs=in_specs, out_specs=out_specs, check_vma=False)
```

```python
import jax
import jax.numpy as jnp
from jax import lax
from jax.experimental import pallas as pl
from jax.experimental.pallas import tpu as pltpu
from jax.sharding import PartitionSpec as P


HEAD = 64
LANES = 128
KEY_CHUNK = 512
RIM = 16
ROWS = 16
OFFSETS = (0, 1, 3, 2)
LOG2E = 1.4426950408889634

epsilon = 1e-05
big_negative = -1e30


VMEM = pl.BlockSpec(memory_space=pltpu.VMEM)
SMEM = pl.BlockSpec(memory_space=pltpu.SMEM)
HBM = pl.BlockSpec(memory_space=pltpu.HBM)


def coords(index):
    b, g = divmod(index, 16)
    return g // 4, (g // 2) % 2, g % 2, b // 2, b % 2


def flat(x, yh, core, z, yl):
    return ((z % 8) * 2 + yl) * 16 + (x % 4) * 4 + yh * 2 + core


def send(value, target):
    pairs = []
    for source in range(256):
        to = target(*coords(source))
        if to is not None:
            pairs.append((source, to if isinstance(to, int) else flat(*to)))
    return lax.ppermute(value, ("blk", "grp"), pairs)


def normalize(values, row_gain):
    center = values - jnp.mean(values, axis=-1, keepdims=True)
    spread = jnp.mean(center * center, axis=-1, keepdims=True)
    return center * lax.rsqrt(spread + epsilon) * row_gain


def low_lanes(rows):
    return lax.broadcasted_iota(jnp.int32, (rows, LANES), 1) < HEAD


def swap_lanes(values):
    return pltpu.roll(values, HEAD, 1)


def project_kernel(slot_ref, own_ref, other_ref, gain_ref, *refs):
    shards, out, normed = refs[:8], refs[8], refs[9]
    rows = own_ref.shape[0]
    gain = gain_ref[0:1, :]
    normed[:rows] = normalize(own_ref[...].astype(jnp.float32), gain).astype(jnp.bfloat16)
    normed[rows:] = normalize(other_ref[...].astype(jnp.float32), gain).astype(jnp.bfloat16)
    low = low_lanes(rows)
    contract = (((1,), (1,)), ((), ()))
    for pair in range(4):
        weights = jnp.concatenate(
            [shards[i][HEAD : 2 * HEAD, :] for i in (2 * pair, 2 * pair + 1)], axis=0
        )
        both = lax.dot_general(normed[...], weights, contract, preferred_element_type=jnp.float32)
        own, other = both[:rows], both[rows:]
        out[slot_ref[2 * pair], :rows] = jnp.where(low, own, swap_lanes(other)).astype(jnp.bfloat16)
        out[slot_ref[2 * pair + 1], :rows] = jnp.where(low, swap_lanes(own), other).astype(jnp.bfloat16)
        for i in (2 * pair, 2 * pair + 1):
            weights = jnp.concatenate([shards[i][2 * HEAD :, :], shards[i][:HEAD, :]], axis=0)
            flipped = lax.dot_general(
                weights, normed[...], contract, preferred_element_type=jnp.float32
            )
            value = flipped[:HEAD].astype(jnp.bfloat16)
            query = (flipped[HEAD:] * (HEAD**-0.5 * LOG2E)).astype(jnp.bfloat16)
            for part, flat_part in enumerate((value, query)):
                for j in range(2 * rows // LANES):
                    at = (part + 1) * rows + j * HEAD
                    out[slot_ref[i], at : at + HEAD] = flat_part[:, j * LANES : (j + 1) * LANES]


def project_qkv(slots, own, other, gain, shards):
    rows, width = own.shape
    return pl.pallas_call(
        project_kernel,
        out_shape=jax.ShapeDtypeStruct((8, 3 * rows, LANES), jnp.bfloat16),
        in_specs=[SMEM] + [VMEM] * 11,
        out_specs=VMEM,
        scratch_shapes=[pltpu.VMEM((2 * rows, width), jnp.bfloat16)],
        compiler_params=pltpu.CompilerParams(vmem_limit_bytes=24 * 1024 * 1024),
    )(slots, own, other, gain, *shards)


def attend_kernel(base_ref, lo_ref, hi_ref, start_ref, end_ref, in_ref, out_ref, *scratch):
    keys, values, queries, scores, most_ref = scratch
    sources = in_ref.shape[0]
    block = in_ref.shape[1] // 3
    lo, hi = lo_ref[0:1, :], hi_ref[0:1, :]
    low = low_lanes(block)
    row = lax.broadcasted_iota(jnp.int32, (block, LANES), 0)
    place = lax.broadcasted_iota(jnp.int32, (16, block), 0)
    column = lax.broadcasted_iota(jnp.int32, (16, block), 1)
    start, end = jnp.zeros_like(place), jnp.zeros_like(place)
    for u in range(start_ref.shape[0]):
        start, end = jnp.where(place == u, start_ref[u], start), jnp.where(place == u, end_ref[u], end)
    window = keys.shape[0]
    extra = values.shape[1] - HEAD
    top = lax.broadcasted_iota(jnp.int32, (extra, KEY_CHUNK), 0) == 0
    for j in range(values.shape[0]):
        values[j, HEAD:] = jnp.where(top, 1.0, 0.0).astype(jnp.bfloat16)

    def prepare(s, carry):
        key = in_ref[s, :block].astype(jnp.float32)
        for side in range(2):
            base = base_ref[side] + s * (2 * block)
            inside = (row + base >= lo) & (row + base < hi)
            at = pl.ds(pl.multiple_of((2 * s + side) * block, block), block)
            mask = jnp.where(inside, 0.0, big_negative)
            keys[at, :] = jnp.where(low, swap_lanes(key) if side else key, mask).astype(jnp.bfloat16)
            mark = jnp.where((column + base >= start) & (column + base < end), 1.0, 0.0)
            queries[2 * s + side, HEAD : HEAD + 16] = mark.astype(jnp.bfloat16)
            queries[2 * s + side, HEAD + 16 :] = jnp.zeros((HEAD - 16, block), jnp.bfloat16)
        for i in range(2 * block // LANES):
            at = block + i * HEAD
            values[s, :HEAD, i * LANES : (i + 1) * LANES] = in_ref[s, at : at + HEAD]
            side, part = divmod(i * LANES, block)
            at += block
            queries[2 * s + side, :HEAD, part : part + LANES] = in_ref[s, at : at + HEAD]
        return carry

    lax.fori_loop(0, sources, prepare, 0)
    chunks = window // KEY_CHUNK

    def score(query, j):
        at = slice(j * KEY_CHUNK, (j + 1) * KEY_CHUNK)
        return jnp.dot(keys[at, :], query, preferred_element_type=jnp.float32)

    def weigh(j, most):
        probs = jnp.exp2(scores[j * KEY_CHUNK : (j + 1) * KEY_CHUNK, :] - most)
        return jnp.dot(values[j], probs.astype(jnp.bfloat16), preferred_element_type=jnp.float32)

    def finish(total, i):
        mixed = total[:HEAD] / total[HEAD : HEAD + 1]
        side = lax.rem(i, 2)
        out_ref[i - side + base_ref[2 + side]] = mixed.astype(jnp.bfloat16)

    def step(i, carry):
        query = queries[i]
        most = most_ref[0:1, :]
        best, total = None, None
        for j in range(chunks):
            part = weigh(j, most)
            total = part if total is None else total + part
            part = score(query, j)
            scores[j * KEY_CHUNK : (j + 1) * KEY_CHUNK, :] = part
            part = jnp.max(part.reshape(KEY_CHUNK // 8, 8, block), axis=0)
            best = part if best is None else jnp.maximum(best, part)
        most_ref[...] = jnp.broadcast_to(jnp.max(best, axis=0, keepdims=True), (8, block))
        finish(total, jnp.maximum(i - 1, 0))
        return carry

    lax.fori_loop(0, 2 * sources, step, 0)
    total = None
    for j in range(chunks):
        part = weigh(j, most_ref[0:1, :])
        total = part if total is None else total + part
    finish(total, 2 * sources - 1)


def attend(bases, lo, hi, starts, ends, parts):
    sources, block = parts.shape[0], parts.shape[1] // 3
    window = 2 * block * sources
    return pl.pallas_call(
        attend_kernel,
        out_shape=jax.ShapeDtypeStruct((2 * sources, HEAD, block), jnp.bfloat16),
        in_specs=[SMEM] + [VMEM] * 2 + [SMEM] * 2 + [VMEM],
        out_specs=VMEM,
        scratch_shapes=[
            pltpu.VMEM((window, LANES), jnp.bfloat16),
            pltpu.VMEM((window // KEY_CHUNK, HEAD + 16, KEY_CHUNK), jnp.bfloat16),
            pltpu.VMEM((2 * sources, LANES, block), jnp.bfloat16),
        ]
        + [pltpu.VMEM((window, block), jnp.float32), pltpu.VMEM((8, block), jnp.float32)],
        compiler_params=pltpu.CompilerParams(vmem_limit_bytes=24 * 1024 * 1024),
    )(bases, lo, hi, starts, ends, parts)


def gate_kernel(mixed, frames, gain, w_out_hbm, w_glu_hbm, residual_ref, gated_ref, *scratch):
    w_out, w_glu, attended, out_sem, glu_sem = scratch
    out_copy = pltpu.make_async_copy(w_out_hbm, w_out, out_sem)
    glu_copy = pltpu.make_async_copy(w_glu_hbm, w_glu, glu_sem)
    out_copy.start()
    glu_copy.start()
    heads = mixed.shape[0]
    for pair in range(heads // 2):
        flipped = jnp.concatenate([mixed[2 * pair], mixed[2 * pair + 1]], axis=0).astype(jnp.float32)
        attended[:, pair * LANES : (pair + 1) * LANES] = flipped.T.astype(jnp.bfloat16)
    out_copy.wait()
    projected = jnp.dot(attended[...], w_out[...], preferred_element_type=jnp.float32)
    residual = (frames[...].astype(jnp.float32) + projected).astype(jnp.bfloat16)
    residual_ref[...] = residual
    width = frames.shape[1]
    conv_in = normalize(residual.astype(jnp.float32), gain[0:1, :]).astype(jnp.bfloat16)
    glu_copy.wait()
    step = 256
    for j in range(0, width, step):
        a = jnp.dot(conv_in, w_glu[:, j : j + step], preferred_element_type=jnp.float32)
        b = jnp.dot(conv_in, w_glu[:, width + j : width + j + step], preferred_element_type=jnp.float32)
        gated_ref[:, j : j + step] = (a * jax.nn.sigmoid(b)).astype(jnp.bfloat16)


def gate(mixed, frames, gain, w_out, w_glu):
    shape = jax.ShapeDtypeStruct(frames.shape, jnp.bfloat16)
    return pl.pallas_call(
        gate_kernel,
        out_shape=[shape, shape],
        in_specs=[VMEM] * 3 + [HBM] * 2,
        out_specs=[VMEM] * 2,
        scratch_shapes=[
            pltpu.VMEM(w_out.shape, jnp.bfloat16),
            pltpu.VMEM(w_glu.shape, jnp.bfloat16),
            pltpu.VMEM(frames.shape, jnp.bfloat16),
            pltpu.SemaphoreType.DMA,
            pltpu.SemaphoreType.DMA,
        ],
        compiler_params=pltpu.CompilerParams(vmem_limit_bytes=24 * 1024 * 1024),
    )(mixed, frames, gain, w_out, w_glu)


def convolve(source, row, weights, t_first, t_last, position, start_ref, end_ref, masked):
    place = lax.broadcasted_iota(jnp.int32, (ROWS, LANES), 0) + position
    lo, hi = jnp.zeros_like(place), jnp.zeros_like(place)
    if masked:
        for u in range(start_ref.shape[0]):
            inside = (place >= start_ref[u]) & (place < end_ref[u])
            lo, hi = jnp.where(inside, start_ref[u], lo), jnp.where(inside, end_ref[u], hi)
        lo, hi = lo - place, hi - place
    tiles = source.shape[0]
    totals = [None] * tiles
    for t in range(t_first, t_last):
        same = (lo <= t - RIM + 1) & (hi > t - RIM + 1) if masked else None
        for c in range(tiles):
            term = source[c, pl.ds(row + t + 1, ROWS), :] * weights[t : t + 1, c * LANES : (c + 1) * LANES]
            term = jnp.where(same, term, 0.0) if masked else term
            totals[c] = term if totals[c] is None else totals[c] + term
    return totals


def inner_kernel(first_ref, start_ref, end_ref, gated, weights, out, padded):
    rows, width = gated.shape
    for c in range(width // LANES):
        padded[c, :RIM] = jnp.zeros((RIM, LANES), jnp.float32)
        padded[c, RIM : RIM + rows] = gated[:, c * LANES : (c + 1) * LANES].astype(jnp.float32)
        padded[c, RIM + rows :] = jnp.zeros((RIM, LANES), jnp.float32)

    def step(i, carry):
        row = pl.multiple_of(i * ROWS, ROWS)
        position = first_ref[0] + row
        crossed = False
        for u in range(1, start_ref.shape[0]):
            crossed |= (start_ref[u] > position - RIM) & (start_ref[u] < position + ROWS + RIM)

        def run(masked):
            totals = convolve(
                padded, row, weights, 0, weights.shape[0], position, start_ref, end_ref, masked
            )
            for c, total in enumerate(totals):
                out[pl.ds(row, ROWS), c * LANES : (c + 1) * LANES] = total

        pl.when(crossed)(lambda: run(True))
        pl.when(jnp.logical_not(crossed))(lambda: run(False))
        return carry

    lax.fori_loop(0, rows // ROWS, step, 0)


def convolve_inner(first, starts, ends, gated, weights):
    rows, width = gated.shape
    return pl.pallas_call(
        inner_kernel,
        out_shape=jax.ShapeDtypeStruct(gated.shape, jnp.float32),
        in_specs=[SMEM] * 3 + [VMEM] * 2,
        out_specs=VMEM,
        scratch_shapes=[pltpu.VMEM((width // LANES, rows + 2 * RIM, LANES), jnp.float32)],
        compiler_params=pltpu.CompilerParams(vmem_limit_bytes=16 * 1024 * 1024),
    )(first, starts, ends, gated, weights)


def last_kernel(
    first_ref, start_ref, end_ref, inner, left, right, residual, weights, gain, w_proj_hbm, out, *scratch
):
    w_proj, total, edge, sem = scratch
    copy = pltpu.make_async_copy(w_proj_hbm, w_proj, sem)
    copy.start()
    rows, width = inner.shape
    total[...] = inner[...]
    count = weights.shape[0]
    for side, rim in enumerate((left, right)):
        at = 0 if side == 0 else 2 * RIM
        row = 0 if side == 0 else rows - ROWS
        for c in range(width // LANES):
            edge[c] = jnp.zeros(edge.shape[1:], jnp.float32)
            edge[c, at : at + RIM] = rim[:, c * LANES : (c + 1) * LANES].astype(jnp.float32)
        span = (0, RIM - 1) if side == 0 else (RIM, count)
        parts = convolve(
            edge, 0, weights, *span, first_ref[0] + row, start_ref, end_ref, True
        )
        for c, part in enumerate(parts):
            lanes = slice(c * LANES, (c + 1) * LANES)
            total[row : row + ROWS, lanes] = total[row : row + ROWS, lanes] + part
    normed = normalize(total[...], gain[0:1, :])
    activated = (normed * jax.nn.sigmoid(normed)).astype(jnp.bfloat16)
    copy.wait()
    projected = jnp.dot(activated, w_proj[...], preferred_element_type=jnp.float32)
    out[...] = (residual[...].astype(jnp.float32) + projected).astype(jnp.bfloat16)


def finish_block(first, starts, ends, inner, left, right, residual, weights, gain, w_proj):
    _, width = inner.shape
    return pl.pallas_call(
        last_kernel,
        out_shape=jax.ShapeDtypeStruct(residual.shape, jnp.bfloat16),
        in_specs=[SMEM] * 3 + [VMEM] * 6 + [HBM],
        out_specs=VMEM,
        scratch_shapes=[
            pltpu.VMEM(w_proj.shape, jnp.bfloat16),
            pltpu.VMEM(inner.shape, jnp.float32),
            pltpu.VMEM((width // LANES, 3 * RIM, LANES), jnp.float32),
            pltpu.SemaphoreType.DMA,
        ],
        compiler_params=pltpu.CompilerParams(vmem_limit_bytes=24 * 1024 * 1024),
    )(first, starts, ends, inner, left, right, residual, weights, gain, w_proj)


def body(
    frames, utt_lengths, attn_gain, w_qkv, w_out, conv_gain, w_glu, w_depth, depth_gain, w_proj
):
    frame_rows = frames.shape[1]
    block_index = lax.axis_index("blk")
    group_index = lax.axis_index("grp")
    yl = block_index % 2
    x, core = group_index // 4, group_index % 2
    window_start = group_index * (16 * frame_rows)
    first_frame = window_start + block_index * frame_rows
    local_frames = frames[0]

    other_frames = send(local_frames, lambda x, yh, c, z, yl: (x, yh, c, z, 1 - yl))
    shard = w_qkv.T

    def route(offset):
        return lambda x, yh, c, z, yl: (
            (x - offset, yh, yh, z, c) if yl == c else (x - offset, 1 - yh, yh, z, c)
        )

    near = [send(shard, route(offset)) for offset in OFFSETS]
    swap = lambda x, yh, c, z, yl: (x, yh, 1 - c, z, yl)
    far = [send(piece, swap) for piece in near]
    slots = jnp.stack([2 * ((x + offset) % 4) + c for c in (core, 1 - core) for offset in OFFSETS])
    parts = project_qkv(slots, local_frames, other_frames, attn_gain[None, :], near + far)
    groups = [[2 * z + yl for z in range(8)] for yl in range(2)]
    parts = lax.all_to_all(parts, "blk", 0, 0, axis_index_groups=groups, tiled=True)
    ends = jnp.cumsum(utt_lengths)
    starts = ends - utt_lengths
    pad = (HEAD, HEAD - utt_lengths.shape[0])
    sides = jnp.stack([yl, 1 - yl])
    bases = jnp.concatenate([window_start + sides * frame_rows, sides])
    lo, hi = jnp.pad(starts, pad)[None, :], jnp.pad(ends, pad)[None, :]
    mixed = attend(bases, lo, hi, starts, ends, parts)
    mixed = lax.all_to_all(mixed, "blk", 0, 0, tiled=True)
    residual, gated = gate(mixed, local_frames, conv_gain[None, :], w_out, w_glu)

    def neighbour(step):
        def target(x, yh, c, z, yl):
            place = (x * 4 + yh * 2 + c) * 16 + z * 2 + yl + step
            return (place % 16) * 16 + place // 16 if 0 <= place < 256 else None

        return target

    left = send(gated[frame_rows - RIM :], neighbour(1))
    right = send(gated[:RIM], neighbour(-1))
    where = (first_frame[None], starts, ends)
    inner = convolve_inner(*where, gated, w_depth)
    result = finish_block(*where, inner, left, right, residual, w_depth, depth_gain[None, :], w_proj)
    return result[None]


def solution(mesh):
    in_specs = (P("grp", "blk", None), P(), P(), P(None, "grp"), P(), P(), P(), P(), P(), P())
    out_specs = P("grp", "blk", None)
    return jax.shard_map(body, mesh=mesh, in_specs=in_specs, out_specs=out_specs, check_vma=False)
```

```python
import jax
import jax.numpy as jnp
from jax import lax
from jax.experimental import pallas as pl
from jax.experimental.pallas import tpu as pltpu
from jax.sharding import PartitionSpec as P


HEAD = 64
LANES = 128
KEY_CHUNK = 512
RIM = 16
ROWS = 16
OFFSETS = (0, 1, 3, 2)
SEND_ORDER = (4, 3, 5, 2, 6, 1, 7)
LOG2E = 1.4426950408889634

epsilon = 1e-05
big_negative = -1e30


VMEM = pl.BlockSpec(memory_space=pltpu.VMEM)
SMEM = pl.BlockSpec(memory_space=pltpu.SMEM)
HBM = pl.BlockSpec(memory_space=pltpu.HBM)


def coords(index):
    b, g = divmod(index, 16)
    return g // 4, (g // 2) % 2, g % 2, b // 2, b % 2


def flat(x, yh, core, z, yl):
    return ((z % 8) * 2 + yl) * 16 + (x % 4) * 4 + yh * 2 + core


def send(value, target):
    pairs = []
    for source in range(256):
        to = target(*coords(source))
        if to is not None:
            pairs.append((source, to if isinstance(to, int) else flat(*to)))
    return lax.ppermute(value, ("blk", "grp"), pairs)


def normalize(values, row_gain):
    center = values - jnp.mean(values, axis=-1, keepdims=True)
    spread = jnp.mean(center * center, axis=-1, keepdims=True)
    return center * lax.rsqrt(spread + epsilon) * row_gain


def low_lanes(rows):
    return lax.broadcasted_iota(jnp.int32, (rows, LANES), 1) < HEAD


def swap_lanes(values):
    return pltpu.roll(values, HEAD, 1)


X, CORE, Z, YL, WINDOW, FIRST = range(6)


def shard_head(me, i):
    core = me[CORE] if i < 4 else 1 - me[CORE]
    return 2 * lax.rem(me[X] + OFFSETS[i % 4], 4) + core


def inside(position, start_ref, end_ref, place):
    start, end = jnp.zeros_like(position), jnp.zeros_like(position)
    for u in range(start_ref.shape[0]):
        start, end = jnp.where(place == u, start_ref[u], start), jnp.where(place == u, end_ref[u], end)
    return (position >= start) & (position < end)


CONTRACT = (((1,), (1,)), ((), ()))


def transposed(out, index, start, flipped):
    for j in range(flipped.shape[1] // LANES):
        at = start + j * HEAD
        out[index, at : at + HEAD] = flipped[:, j * LANES : (j + 1) * LANES].astype(jnp.bfloat16)


def key_value_kernel(me, own_hbm, gain_hbm, other_hbm, *refs):
    shards_hbm, out, normed = refs[:8], refs[8], refs[9]
    own_ref, gain_ref, other_ref, shards, sems = refs[10:]
    pairs = [(own_hbm, own_ref), (gain_hbm, gain_ref), (other_hbm, other_ref)]
    pairs += [(shards_hbm[i], shards.at[i]) for i in range(8)]
    copies = [pltpu.make_async_copy(a, b, sems.at[i]) for i, (a, b) in enumerate(pairs)]
    for copy in copies:
        copy.start()
    copies[1].wait()
    rows = own_ref.shape[0]
    gain = gain_ref[0:1, :]
    copies[0].wait()
    normed[:rows] = normalize(own_ref[...].astype(jnp.float32), gain).astype(jnp.bfloat16)
    copies[2].wait()
    normed[rows:] = normalize(other_ref[...].astype(jnp.float32), gain).astype(jnp.bfloat16)
    low = low_lanes(rows)
    for i in range(0, 8, 2):
        copies[3 + i].wait()
        copies[4 + i].wait()
        heads = shard_head(me, i), shard_head(me, i + 1)
        weights = jnp.concatenate([shards[i, :HEAD], shards[i + 1, :HEAD]], axis=0)
        both = lax.dot_general(normed[...], weights, CONTRACT, preferred_element_type=jnp.float32)
        own, other = both[:rows], both[rows:]
        out[heads[0], :rows] = jnp.where(low, own, swap_lanes(other)).astype(jnp.bfloat16)
        out[heads[1], :rows] = jnp.where(low, swap_lanes(own), other).astype(jnp.bfloat16)
        weights = jnp.concatenate([shards[i, HEAD:], shards[i + 1, HEAD:]], axis=0)
        both = lax.dot_general(weights, normed[...], CONTRACT, preferred_element_type=jnp.float32)
        transposed(out, heads[0], rows, both[:HEAD])
        transposed(out, heads[1], rows, both[HEAD:])


def project_key_value(me, own, other, gain, shards):
    rows, width = own.shape
    return pl.pallas_call(
        key_value_kernel,
        out_shape=[
            jax.ShapeDtypeStruct((8, 2 * rows, LANES), jnp.bfloat16),
            jax.ShapeDtypeStruct((2 * rows, width), jnp.bfloat16),
        ],
        in_specs=[SMEM] + [HBM] * 11,
        out_specs=[VMEM] * 2,
        scratch_shapes=[
            pltpu.VMEM(own.shape, jnp.bfloat16),
            pltpu.VMEM(gain.shape, jnp.float32),
            pltpu.VMEM(own.shape, jnp.bfloat16),
            pltpu.VMEM((8,) + shards[0].shape, jnp.bfloat16),
            pltpu.SemaphoreType.DMA((11,)),
        ],
        compiler_params=pltpu.CompilerParams(vmem_limit_bytes=60 * 1024 * 1024),
    )(me, own, gain, other, *shards)


def query_kernel(me, normed, *refs):
    near, far, outs, staged = refs[:4], refs[4], refs[5:13], refs[13]
    shards = [ref[...] for ref in near] + [far[i * HEAD : (i + 1) * HEAD, :] for i in range(4)]
    for i in range(0, 8, 2):
        weights = jnp.concatenate([shards[i], shards[i + 1]], axis=0)
        both = lax.dot_general(weights, normed[...], CONTRACT, preferred_element_type=jnp.float32)
        both = both * (HEAD**-0.5 * LOG2E)
        transposed(staged, lax.rem(shard_head(me, i) + 8 - me[Z], 8), 0, both[:HEAD])
        transposed(staged, lax.rem(shard_head(me, i + 1) + 8 - me[Z], 8), 0, both[HEAD:])
    for d in range(8):
        outs[d][...] = staged[d]


def project_query(me, normed, shards):
    shape = (normed.shape[0] // 2, LANES)
    return pl.pallas_call(
        query_kernel,
        out_shape=[jax.ShapeDtypeStruct(shape, jnp.bfloat16)] * 8,
        in_specs=[SMEM] + [VMEM] * 6,
        out_specs=[VMEM] * 8,
        scratch_shapes=[pltpu.VMEM((8,) + shape, jnp.bfloat16)],
        compiler_params=pltpu.CompilerParams(vmem_limit_bytes=16 * 1024 * 1024),
    )(me, normed, *shards)


def attend_kernel(me, start_ref, end_ref, in_ref, *refs):
    parts_hbm, out_ref = refs[:8], refs[8]
    keys, values, queries, scores, most_ref, parts_q, sems = refs[9:]
    copies = [pltpu.make_async_copy(parts_hbm[d], parts_q.at[d], sems.at[d]) for d in range(8)]
    for copy in copies:
        copy.start()
    sources = in_ref.shape[0]
    block = in_ref.shape[1] // 2
    low = low_lanes(block)
    row = lax.broadcasted_iota(jnp.int32, (block, LANES), 0)
    lane = lax.broadcasted_iota(jnp.int32, (block, LANES), 1) - HEAD
    place = lax.broadcasted_iota(jnp.int32, (16, block), 0)
    column = lax.broadcasted_iota(jnp.int32, (16, block), 1)
    window = keys.shape[0]
    top = lax.broadcasted_iota(jnp.int32, (values.shape[1] - HEAD, KEY_CHUNK), 0) == 0
    for j in range(values.shape[0]):
        values[j, HEAD:] = jnp.where(top, 1.0, 0.0).astype(jnp.bfloat16)

    def prepare(s, carry):
        key = in_ref[s, :block].astype(jnp.float32)
        for side in range(2):
            shard = 2 * s + (me[YL] if side == 0 else 1 - me[YL])
            base = me[WINDOW] + shard * block
            at = pl.ds(pl.multiple_of((2 * s + side) * block, block), block)
            mask = jnp.where(inside(row + base, start_ref, end_ref, lane), 0.0, big_negative)
            keys[at, :] = jnp.where(low, swap_lanes(key) if side else key, mask).astype(jnp.bfloat16)
        for i in range(2 * block // LANES):
            at = block + i * HEAD
            values[s, :HEAD, i * LANES : (i + 1) * LANES] = in_ref[s, at : at + HEAD]
        return carry

    def origin(i):
        d, side = i // 2, lax.rem(i, 2)
        shard = jnp.where(side == 0, me[YL], 1 - me[YL])
        return 2 * lax.rem(me[Z] + 8 - d, 8) + shard

    for i in range(2 * sources):
        if i % 2 == 0:
            copies[i // 2].wait()
        mark = inside(column + (me[WINDOW] + origin(i) * block), start_ref, end_ref, place)
        queries[i, HEAD : HEAD + 16] = jnp.where(mark, 1.0, 0.0).astype(jnp.bfloat16)
        queries[i, HEAD + 16 :] = jnp.zeros((HEAD - 16, block), jnp.bfloat16)
        for j in range(block // LANES):
            at = ((i % 2) * (block // LANES) + j) * HEAD
            queries[i, :HEAD, j * LANES : (j + 1) * LANES] = parts_q[i // 2, at : at + HEAD]
    lax.fori_loop(0, sources, prepare, 0)
    chunks = window // KEY_CHUNK

    def score(query, j):
        at = slice(j * KEY_CHUNK, (j + 1) * KEY_CHUNK)
        return jnp.dot(keys[at, :], query, preferred_element_type=jnp.float32)

    def weigh(j, most):
        probs = jnp.exp2(scores[j * KEY_CHUNK : (j + 1) * KEY_CHUNK, :] - most)
        return jnp.dot(values[j], probs.astype(jnp.bfloat16), preferred_element_type=jnp.float32)

    def finish(total, i):
        mixed = total[:HEAD] / total[HEAD : HEAD + 1]
        out_ref[origin(i)] = mixed.astype(jnp.bfloat16)

    def step(i, carry):
        query = queries[i]
        most = most_ref[0:1, :]
        best, total = None, None
        for j in range(chunks):
            part = weigh(j, most)
            total = part if total is None else total + part
            part = score(query, j)
            scores[j * KEY_CHUNK : (j + 1) * KEY_CHUNK, :] = part
            part = jnp.max(part.reshape(KEY_CHUNK // 8, 8, block), axis=0)
            best = part if best is None else jnp.maximum(best, part)
        most_ref[...] = jnp.broadcast_to(jnp.max(best, axis=0, keepdims=True), (8, block))
        finish(total, jnp.maximum(i - 1, 0))
        return carry

    lax.fori_loop(0, 2 * sources, step, 0)
    total = None
    for j in range(chunks):
        part = weigh(j, most_ref[0:1, :])
        total = part if total is None else total + part
    finish(total, 2 * sources - 1)


def attend(me, starts, ends, key_value, queries):
    sources, block = key_value.shape[0], key_value.shape[1] // 2
    window = 2 * block * sources
    return pl.pallas_call(
        attend_kernel,
        out_shape=jax.ShapeDtypeStruct((2 * sources, HEAD, block), jnp.bfloat16),
        in_specs=[SMEM] * 3 + [VMEM] + [HBM] * 8,
        out_specs=VMEM,
        scratch_shapes=[
            pltpu.VMEM((window, LANES), jnp.bfloat16),
            pltpu.VMEM((window // KEY_CHUNK, HEAD + 16, KEY_CHUNK), jnp.bfloat16),
            pltpu.VMEM((2 * sources, LANES, block), jnp.bfloat16),
        ]
        + [pltpu.VMEM((window, block), jnp.float32), pltpu.VMEM((8, block), jnp.float32)]
        + [pltpu.VMEM((8, block, LANES), jnp.bfloat16), pltpu.SemaphoreType.DMA((8,))],
        compiler_params=pltpu.CompilerParams(vmem_limit_bytes=24 * 1024 * 1024),
    )(me, starts, ends, key_value, *queries)


def gate_kernel(mixed, frames, gain, w_out_hbm, w_glu_hbm, residual_ref, gated_ref, *scratch):
    w_out, w_glu, attended, out_sem, glu_sem = scratch
    out_copy = pltpu.make_async_copy(w_out_hbm, w_out, out_sem)
    glu_copy = pltpu.make_async_copy(w_glu_hbm, w_glu, glu_sem)
    out_copy.start()
    glu_copy.start()
    heads = mixed.shape[0]
    for pair in range(heads // 2):
        flipped = jnp.concatenate([mixed[2 * pair], mixed[2 * pair + 1]], axis=0).astype(jnp.float32)
        attended[:, pair * LANES : (pair + 1) * LANES] = flipped.T.astype(jnp.bfloat16)
    out_copy.wait()
    projected = jnp.dot(attended[...], w_out[...], preferred_element_type=jnp.float32)
    residual = (frames[...].astype(jnp.float32) + projected).astype(jnp.bfloat16)
    residual_ref[...] = residual
    width = frames.shape[1]
    conv_in = normalize(residual.astype(jnp.float32), gain[0:1, :]).astype(jnp.bfloat16)
    glu_copy.wait()
    step = 256
    for j in range(0, width, step):
        a = jnp.dot(conv_in, w_glu[:, j : j + step], preferred_element_type=jnp.float32)
        b = jnp.dot(conv_in, w_glu[:, width + j : width + j + step], preferred_element_type=jnp.float32)
        gated_ref[:, j : j + step] = (a * jax.nn.sigmoid(b)).astype(jnp.bfloat16)


def gate(mixed, frames, gain, w_out, w_glu):
    shape = jax.ShapeDtypeStruct(frames.shape, jnp.bfloat16)
    return pl.pallas_call(
        gate_kernel,
        out_shape=[shape, shape],
        in_specs=[VMEM] * 3 + [HBM] * 2,
        out_specs=[VMEM] * 2,
        scratch_shapes=[
            pltpu.VMEM(w_out.shape, jnp.bfloat16),
            pltpu.VMEM(w_glu.shape, jnp.bfloat16),
            pltpu.VMEM(frames.shape, jnp.bfloat16),
            pltpu.SemaphoreType.DMA,
            pltpu.SemaphoreType.DMA,
        ],
        compiler_params=pltpu.CompilerParams(vmem_limit_bytes=58 * 1024 * 1024),
    )(mixed, frames, gain, w_out, w_glu)


def convolve(source, row, weights, t_first, t_last, position, start_ref, end_ref, masked):
    place = lax.broadcasted_iota(jnp.int32, (ROWS, LANES), 0) + position
    lo, hi = jnp.zeros_like(place), jnp.zeros_like(place)
    if masked:
        for u in range(start_ref.shape[0]):
            inside = (place >= start_ref[u]) & (place < end_ref[u])
            lo, hi = jnp.where(inside, start_ref[u], lo), jnp.where(inside, end_ref[u], hi)
        lo, hi = lo - place, hi - place
    tiles = source.shape[0]
    totals = [None] * tiles
    for t in range(t_first, t_last):
        same = (lo <= t - RIM + 1) & (hi > t - RIM + 1) if masked else None
        for c in range(tiles):
            term = source[c, pl.ds(row + t + 1, ROWS), :] * weights[t : t + 1, c * LANES : (c + 1) * LANES]
            term = jnp.where(same, term, 0.0) if masked else term
            totals[c] = term if totals[c] is None else totals[c] + term
    return totals


def inner_kernel(me, start_ref, end_ref, gated, weights, out, padded):
    rows, width = gated.shape
    for c in range(width // LANES):
        padded[c, :RIM] = jnp.zeros((RIM, LANES), jnp.float32)
        padded[c, RIM : RIM + rows] = gated[:, c * LANES : (c + 1) * LANES].astype(jnp.float32)
        padded[c, RIM + rows :] = jnp.zeros((RIM, LANES), jnp.float32)

    def step(i, carry):
        row = pl.multiple_of(i * ROWS, ROWS)
        position = me[FIRST] + row
        crossed = False
        for u in range(1, start_ref.shape[0]):
            crossed |= (start_ref[u] > position - RIM) & (start_ref[u] < position + ROWS + RIM)

        def run(masked):
            totals = convolve(
                padded, row, weights, 0, weights.shape[0], position, start_ref, end_ref, masked
            )
            for c, total in enumerate(totals):
                out[pl.ds(row, ROWS), c * LANES : (c + 1) * LANES] = total

        pl.when(crossed)(lambda: run(True))
        pl.when(jnp.logical_not(crossed))(lambda: run(False))
        return carry

    lax.fori_loop(0, rows // ROWS, step, 0)


def convolve_inner(me, starts, ends, gated, weights):
    rows, width = gated.shape
    return pl.pallas_call(
        inner_kernel,
        out_shape=jax.ShapeDtypeStruct(gated.shape, jnp.float32),
        in_specs=[SMEM] * 3 + [VMEM] * 2,
        out_specs=VMEM,
        scratch_shapes=[pltpu.VMEM((width // LANES, rows + 2 * RIM, LANES), jnp.float32)],
        compiler_params=pltpu.CompilerParams(vmem_limit_bytes=16 * 1024 * 1024),
    )(me, starts, ends, gated, weights)


def last_kernel(
    me, start_ref, end_ref, inner, left, right, residual, weights, gain, w_proj_hbm, out, *scratch
):
    w_proj, total, edge, sem = scratch
    copy = pltpu.make_async_copy(w_proj_hbm, w_proj, sem)
    copy.start()
    rows, width = inner.shape
    total[...] = inner[...]
    count = weights.shape[0]
    for side, rim in enumerate((left, right)):
        at = 0 if side == 0 else 2 * RIM
        row = 0 if side == 0 else rows - ROWS
        for c in range(width // LANES):
            edge[c] = jnp.zeros(edge.shape[1:], jnp.float32)
            edge[c, at : at + RIM] = rim[:, c * LANES : (c + 1) * LANES].astype(jnp.float32)
        span = (0, RIM - 1) if side == 0 else (RIM, count)
        parts = convolve(
            edge, 0, weights, *span, me[FIRST] + row, start_ref, end_ref, True
        )
        for c, part in enumerate(parts):
            lanes = slice(c * LANES, (c + 1) * LANES)
            total[row : row + ROWS, lanes] = total[row : row + ROWS, lanes] + part
    normed = normalize(total[...], gain[0:1, :])
    activated = (normed * jax.nn.sigmoid(normed)).astype(jnp.bfloat16)
    copy.wait()
    projected = jnp.dot(activated, w_proj[...], preferred_element_type=jnp.float32)
    out[...] = (residual[...].astype(jnp.float32) + projected).astype(jnp.bfloat16)


def finish_block(me, starts, ends, inner, left, right, residual, weights, gain, w_proj):
    _, width = inner.shape
    return pl.pallas_call(
        last_kernel,
        out_shape=jax.ShapeDtypeStruct(residual.shape, jnp.bfloat16),
        in_specs=[SMEM] * 3 + [VMEM] * 6 + [HBM],
        out_specs=VMEM,
        scratch_shapes=[
            pltpu.VMEM(w_proj.shape, jnp.bfloat16),
            pltpu.VMEM(inner.shape, jnp.float32),
            pltpu.VMEM((width // LANES, 3 * RIM, LANES), jnp.float32),
            pltpu.SemaphoreType.DMA,
        ],
        compiler_params=pltpu.CompilerParams(vmem_limit_bytes=24 * 1024 * 1024),
    )(me, starts, ends, inner, left, right, residual, weights, gain, w_proj)


def body(
    frames, utt_lengths, attn_gain, w_qkv, w_out, conv_gain, w_glu, w_depth, depth_gain, w_proj
):
    frame_rows = frames.shape[1]
    block_index = lax.axis_index("blk")
    group_index = lax.axis_index("grp")
    z, yl = block_index // 2, block_index % 2
    x, core = group_index // 4, group_index % 2
    window_start = group_index * (16 * frame_rows)
    first_frame = window_start + block_index * frame_rows
    local_frames = frames[0]
    me = jnp.stack([x, core, z, yl, window_start, first_frame]).astype(jnp.int32)

    shard = w_qkv.T

    def route(offset):
        return lambda x, yh, c, z, yl: (
            (x - offset, yh, yh, z, c) if yl == c else (x - offset, 1 - yh, yh, z, c)
        )

    swap = lambda x, yh, c, z, yl: (x, yh, 1 - c, z, yl)
    across = lambda x, yh, c, z, yl: (x, yh, c, z, 1 - yl)
    near = [send(shard[HEAD:], route(o)) for o in OFFSETS]
    other_frames = send(local_frames, across)
    far = [send(piece, swap) for piece in near]
    near_q = [send(shard[:HEAD], route(o)) for o in OFFSETS]
    far_q = send(jnp.concatenate(near_q, axis=0), swap)
    key_value, normed = project_key_value(me, local_frames, other_frames, attn_gain[None, :], near + far)
    queries = project_query(me, normed, near_q + [far_q])
    groups = [[2 * z + yl for z in range(8)] for yl in range(2)]
    key_value = lax.all_to_all(key_value, "blk", 0, 0, axis_index_groups=groups, tiled=True)
    queries = list(queries)
    for d in SEND_ORDER:
        queries[d] = send(queries[d], lambda x, yh, c, z, yl: (x, yh, c, z + d, yl))
    ends = jnp.cumsum(utt_lengths)
    starts = ends - utt_lengths
    mixed = attend(me, starts, ends, key_value, queries)
    mixed = lax.all_to_all(mixed, "blk", 0, 0, tiled=True)
    residual, gated = gate(mixed, local_frames, conv_gain[None, :], w_out, w_glu)

    def neighbour(step):
        def target(x, yh, c, z, yl):
            place = (x * 4 + yh * 2 + c) * 16 + z * 2 + yl + step
            return (place % 16) * 16 + place // 16 if 0 <= place < 256 else None

        return target

    left = send(gated[frame_rows - RIM :], neighbour(1))
    right = send(gated[:RIM], neighbour(-1))
    where = (me, starts, ends)
    inner = convolve_inner(*where, gated, w_depth)
    result = finish_block(*where, inner, left, right, residual, w_depth, depth_gain[None, :], w_proj)
    return result[None]


def solution(mesh):
    in_specs = (P("grp", "blk", None), P(), P(), P(None, "grp"), P(), P(), P(), P(), P(), P())
    out_specs = P("grp", "blk", None)
    return jax.shard_map(body, mesh=mesh, in_specs=in_specs, out_specs=out_specs, check_vma=False)
```

```python
import functools

import jax
import jax.numpy as jnp
from jax import lax
from jax.experimental import pallas as pl
from jax.experimental.pallas import tpu as pltpu
from jax.sharding import PartitionSpec as P


HEAD = 64
LANES = 128
KEY_CHUNK = 512
RIM = 16
ROWS = 16
OFFSETS = (0, 1, 3, 2)
SEND_ORDER = (1, 7, 2, 6, 3, 5, 4)
PIECES = ((0, 1, 7, 2), (6, 3, 5, 4))
LOG2E = 1.4426950408889634

epsilon = 1e-05
big_negative = -1e30


VMEM = pl.BlockSpec(memory_space=pltpu.VMEM)
SMEM = pl.BlockSpec(memory_space=pltpu.SMEM)
HBM = pl.BlockSpec(memory_space=pltpu.HBM)


def coords(index):
    b, g = divmod(index, 16)
    return g // 4, (g // 2) % 2, g % 2, b // 2, b % 2


def flat(x, yh, core, z, yl):
    return ((z % 8) * 2 + yl) * 16 + (x % 4) * 4 + yh * 2 + core


def send(value, target):
    pairs = []
    for source in range(256):
        to = target(*coords(source))
        if to is not None:
            pairs.append((source, to if isinstance(to, int) else flat(*to)))
    return lax.ppermute(value, ("blk", "grp"), pairs)


def normalize(values, row_gain):
    center = values - jnp.mean(values, axis=-1, keepdims=True)
    spread = jnp.mean(center * center, axis=-1, keepdims=True)
    return center * lax.rsqrt(spread + epsilon) * row_gain


def low_lanes(rows):
    return lax.broadcasted_iota(jnp.int32, (rows, LANES), 1) < HEAD


def swap_lanes(values):
    return pltpu.roll(values, HEAD, 1)


X, CORE, Z, YL, WINDOW, FIRST = range(6)


def shard_head(me, i):
    core = me[CORE] if i < 4 else 1 - me[CORE]
    return 2 * lax.rem(me[X] + OFFSETS[i % 4], 4) + core


def inside(position, start_ref, end_ref, place):
    start, end = jnp.zeros_like(position), jnp.zeros_like(position)
    for u in range(start_ref.shape[0]):
        start, end = jnp.where(place == u, start_ref[u], start), jnp.where(place == u, end_ref[u], end)
    return (position >= start) & (position < end)


CONTRACT = (((1,), (1,)), ((), ()))


def transposed(out, index, start, flipped):
    for j in range(flipped.shape[1] // LANES):
        at = start + j * HEAD
        out[index, at : at + HEAD] = flipped[:, j * LANES : (j + 1) * LANES].astype(jnp.bfloat16)


def project_kernel(me, own_hbm, other_ref, gain_hbm, *refs):
    shards, out, pieces = refs[:8], refs[8], refs[9:17]
    normed, staged, own_ref, gain_ref, sems, in_sems = refs[17:]
    pairs = ((gain_hbm, gain_ref), (own_hbm, own_ref))
    copies = [pltpu.make_async_copy(a, b, in_sems.at[i]) for i, (a, b) in enumerate(pairs)]
    for copy in copies:
        copy.start()
    copies[0].wait()
    rows = own_ref.shape[0]
    gain = gain_ref[0:1, :]
    normed[rows:] = normalize(other_ref[...].astype(jnp.float32), gain).astype(jnp.bfloat16)
    copies[1].wait()
    normed[:rows] = normalize(own_ref[...].astype(jnp.float32), gain).astype(jnp.bfloat16)
    low = low_lanes(rows)
    for i in range(0, 8, 2):
        heads = shard_head(me, i), shard_head(me, i + 1)
        weights = jnp.concatenate([shards[j][HEAD : 2 * HEAD, :] for j in (i, i + 1)], axis=0)
        both = lax.dot_general(normed[...], weights, CONTRACT, preferred_element_type=jnp.float32)
        own, other = both[:rows], both[rows:]
        out[heads[0], :rows] = jnp.where(low, own, swap_lanes(other)).astype(jnp.bfloat16)
        out[heads[1], :rows] = jnp.where(low, swap_lanes(own), other).astype(jnp.bfloat16)
        for j, head in zip((i, i + 1), heads):
            weights = jnp.concatenate([shards[j][2 * HEAD :, :], shards[j][:HEAD, :]], axis=0)
            both = lax.dot_general(weights, normed[...], CONTRACT, preferred_element_type=jnp.float32)
            transposed(out, head, rows, both[:HEAD])
            query = both[HEAD:] * (HEAD**-0.5 * LOG2E)
            transposed(staged, lax.rem(head + 8 - me[Z], 8), 0, query)
    copies = [pltpu.make_async_copy(staged.at[d], pieces[d], sems.at[d]) for d in range(8)]
    for copy in copies:
        copy.start()
    for copy in copies:
        copy.wait()


def project_qkv(me, own, other, gain, shards):
    rows, width = own.shape
    piece = jax.ShapeDtypeStruct((rows, LANES), jnp.bfloat16)
    return pl.pallas_call(
        project_kernel,
        out_shape=[jax.ShapeDtypeStruct((8, 2 * rows, LANES), jnp.bfloat16)] + [piece] * 8,
        in_specs=[SMEM, HBM, VMEM, HBM] + [VMEM] * 8,
        out_specs=[VMEM] + [HBM] * 8,
        scratch_shapes=[
            pltpu.VMEM((2 * rows, width), jnp.bfloat16),
            pltpu.VMEM((8,) + piece.shape, jnp.bfloat16),
            pltpu.VMEM(own.shape, jnp.bfloat16),
            pltpu.VMEM(gain.shape, jnp.float32),
            pltpu.SemaphoreType.DMA((8,)),
            pltpu.SemaphoreType.DMA((2,)),
        ],
        compiler_params=pltpu.CompilerParams(vmem_limit_bytes=59 * 1024 * 1024),
    )(me, own, other, gain, *shards)


def attend_kernel(pieces, me, start_ref, end_ref, in_ref, before, *refs):
    count = len(pieces)
    parts_hbm, out_ref = refs[:count], refs[count]
    keys, values, queries, scores, most_ref, parts_q, sems = refs[count + 1 :]
    copies = [pltpu.make_async_copy(parts_hbm[d], parts_q.at[d], sems.at[d]) for d in range(count)]
    for copy in copies:
        copy.start()
    out_ref[...] = before[...]
    sources = in_ref.shape[0]
    block = in_ref.shape[1] // 2
    low = low_lanes(block)
    row = lax.broadcasted_iota(jnp.int32, (block, LANES), 0)
    lane = lax.broadcasted_iota(jnp.int32, (block, LANES), 1) - HEAD
    place = lax.broadcasted_iota(jnp.int32, (16, block), 0)
    column = lax.broadcasted_iota(jnp.int32, (16, block), 1)
    window = keys.shape[0]
    top = lax.broadcasted_iota(jnp.int32, (values.shape[1] - HEAD, KEY_CHUNK), 0) == 0
    for j in range(values.shape[0]):
        values[j, HEAD:] = jnp.where(top, 1.0, 0.0).astype(jnp.bfloat16)

    def prepare(s, carry):
        key = in_ref[s, :block].astype(jnp.float32)
        for side in range(2):
            shard = 2 * s + (me[YL] if side == 0 else 1 - me[YL])
            base = me[WINDOW] + shard * block
            at = pl.ds(pl.multiple_of((2 * s + side) * block, block), block)
            mask = jnp.where(inside(row + base, start_ref, end_ref, lane), 0.0, big_negative)
            keys[at, :] = jnp.where(low, swap_lanes(key) if side else key, mask).astype(jnp.bfloat16)
        for i in range(2 * block // LANES):
            at = block + i * HEAD
            values[s, :HEAD, i * LANES : (i + 1) * LANES] = in_ref[s, at : at + HEAD]
        return carry

    def origin(i):
        side, d = lax.rem(i, 2), pieces[0]
        for j in range(1, count):
            d = jnp.where(i // 2 == j, pieces[j], d)
        shard = jnp.where(side == 0, me[YL], 1 - me[YL])
        return 2 * lax.rem(me[Z] + 8 - d, 8) + shard

    for i in range(2 * count):
        if i % 2 == 0:
            copies[i // 2].wait()
        mark = inside(column + (me[WINDOW] + origin(i) * block), start_ref, end_ref, place)
        queries[i, HEAD : HEAD + 16] = jnp.where(mark, 1.0, 0.0).astype(jnp.bfloat16)
        queries[i, HEAD + 16 :] = jnp.zeros((HEAD - 16, block), jnp.bfloat16)
        for j in range(block // LANES):
            at = ((i % 2) * (block // LANES) + j) * HEAD
            queries[i, :HEAD, j * LANES : (j + 1) * LANES] = parts_q[i // 2, at : at + HEAD]
    lax.fori_loop(0, sources, prepare, 0)
    chunks = window // KEY_CHUNK

    def score(query, j):
        at = slice(j * KEY_CHUNK, (j + 1) * KEY_CHUNK)
        return jnp.dot(keys[at, :], query, preferred_element_type=jnp.float32)

    def weigh(j, most):
        probs = jnp.exp2(scores[j * KEY_CHUNK : (j + 1) * KEY_CHUNK, :] - most)
        return jnp.dot(values[j], probs.astype(jnp.bfloat16), preferred_element_type=jnp.float32)

    def finish(total, i):
        mixed = total[:HEAD] / total[HEAD : HEAD + 1]
        out_ref[origin(i)] = mixed.astype(jnp.bfloat16)

    def step(i, carry):
        query = queries[i]
        most = most_ref[0:1, :]
        best, total = None, None
        for j in range(chunks):
            part = weigh(j, most)
            total = part if total is None else total + part
            part = score(query, j)
            scores[j * KEY_CHUNK : (j + 1) * KEY_CHUNK, :] = part
            part = jnp.max(part.reshape(KEY_CHUNK // 8, 8, block), axis=0)
            best = part if best is None else jnp.maximum(best, part)
        most_ref[...] = jnp.broadcast_to(jnp.max(best, axis=0, keepdims=True), (8, block))
        finish(total, jnp.maximum(i - 1, 0))
        return carry

    lax.fori_loop(0, 2 * count, step, 0)
    total = None
    for j in range(chunks):
        part = weigh(j, most_ref[0:1, :])
        total = part if total is None else total + part
    finish(total, 2 * count - 1)


def attend(pieces, me, starts, ends, key_value, before, queries):
    sources, block = key_value.shape[0], key_value.shape[1] // 2
    window, count = 2 * block * sources, len(pieces)
    return pl.pallas_call(
        functools.partial(attend_kernel, pieces),
        out_shape=jax.ShapeDtypeStruct((2 * sources, HEAD, block), jnp.bfloat16),
        in_specs=[SMEM] * 3 + [VMEM] * 2 + [HBM] * count,
        out_specs=VMEM,
        scratch_shapes=[
            pltpu.VMEM((window, LANES), jnp.bfloat16),
            pltpu.VMEM((window // KEY_CHUNK, HEAD + 16, KEY_CHUNK), jnp.bfloat16),
            pltpu.VMEM((2 * count, LANES, block), jnp.bfloat16),
            pltpu.VMEM((window, block), jnp.float32),
            pltpu.VMEM((8, block), jnp.float32),
            pltpu.VMEM((count, block, LANES), jnp.bfloat16),
            pltpu.SemaphoreType.DMA((count,)),
        ],
        compiler_params=pltpu.CompilerParams(vmem_limit_bytes=24 * 1024 * 1024),
    )(me, starts, ends, key_value, before, *queries)


PIECE_COUNT = 4


def copy_rows(source, target, sems):
    step = source.shape[0] // PIECE_COUNT
    at = [pl.ds(i * step, step) for i in range(PIECE_COUNT)]
    copies = [pltpu.make_async_copy(source.at[a], target.at[a], sems.at[i]) for i, a in enumerate(at)]
    for copy in copies:
        copy.start()
    return copies


def wait_all(copies):
    for copy in copies:
        copy.wait()


def gate_kernel(mixed, frames, gain, w_out_hbm, w_glu_hbm, residual_ref, gated_ref, *scratch):
    w_out, w_glu, attended, out_sem, glu_sem = scratch
    out_copies = copy_rows(w_out_hbm, w_out, out_sem)
    glu_copies = copy_rows(w_glu_hbm, w_glu, glu_sem)
    heads = mixed.shape[0]
    for pair in range(heads // 2):
        flipped = jnp.concatenate([mixed[2 * pair], mixed[2 * pair + 1]], axis=0).astype(jnp.float32)
        attended[:, pair * LANES : (pair + 1) * LANES] = flipped.T.astype(jnp.bfloat16)
    wait_all(out_copies)
    projected = jnp.dot(attended[...], w_out[...], preferred_element_type=jnp.float32)
    residual = (frames[...].astype(jnp.float32) + projected).astype(jnp.bfloat16)
    residual_ref[...] = residual
    width = frames.shape[1]
    conv_in = normalize(residual.astype(jnp.float32), gain[0:1, :]).astype(jnp.bfloat16)
    wait_all(glu_copies)
    step = 256
    for j in range(0, width, step):
        a = jnp.dot(conv_in, w_glu[:, j : j + step], preferred_element_type=jnp.float32)
        b = jnp.dot(conv_in, w_glu[:, width + j : width + j + step], preferred_element_type=jnp.float32)
        gated_ref[:, j : j + step] = (a * jax.nn.sigmoid(b)).astype(jnp.bfloat16)


def gate(mixed, frames, gain, w_out, w_glu):
    shape = jax.ShapeDtypeStruct(frames.shape, jnp.bfloat16)
    return pl.pallas_call(
        gate_kernel,
        out_shape=[shape, shape],
        in_specs=[VMEM] * 3 + [HBM] * 2,
        out_specs=[VMEM] * 2,
        scratch_shapes=[
            pltpu.VMEM(w_out.shape, jnp.bfloat16),
            pltpu.VMEM(w_glu.shape, jnp.bfloat16),
            pltpu.VMEM(frames.shape, jnp.bfloat16),
            pltpu.SemaphoreType.DMA((PIECE_COUNT,)),
            pltpu.SemaphoreType.DMA((PIECE_COUNT,)),
        ],
        compiler_params=pltpu.CompilerParams(vmem_limit_bytes=58 * 1024 * 1024),
    )(mixed, frames, gain, w_out, w_glu)


def convolve(source, row, weights, t_first, t_last, position, start_ref, end_ref, masked):
    place = lax.broadcasted_iota(jnp.int32, (ROWS, LANES), 0) + position
    lo, hi = jnp.zeros_like(place), jnp.zeros_like(place)
    if masked:
        for u in range(start_ref.shape[0]):
            inside = (place >= start_ref[u]) & (place < end_ref[u])
            lo, hi = jnp.where(inside, start_ref[u], lo), jnp.where(inside, end_ref[u], hi)
        lo, hi = lo - place, hi - place
    tiles = source.shape[0]
    totals = [None] * tiles
    for t in range(t_first, t_last):
        same = (lo <= t - RIM + 1) & (hi > t - RIM + 1) if masked else None
        for c in range(tiles):
            term = source[c, pl.ds(row + t + 1, ROWS), :] * weights[t : t + 1, c * LANES : (c + 1) * LANES]
            term = jnp.where(same, term, 0.0) if masked else term
            totals[c] = term if totals[c] is None else totals[c] + term
    return totals


def inner_kernel(me, start_ref, end_ref, gated_hbm, weights, out, padded, gated, sems):
    wait_all(copy_rows(gated_hbm, gated, sems))
    rows, width = gated.shape
    for c in range(width // LANES):
        padded[c, :RIM] = jnp.zeros((RIM, LANES), jnp.float32)
        padded[c, RIM : RIM + rows] = gated[:, c * LANES : (c + 1) * LANES].astype(jnp.float32)
        padded[c, RIM + rows :] = jnp.zeros((RIM, LANES), jnp.float32)

    def step(i, carry):
        row = pl.multiple_of(i * ROWS, ROWS)
        position = me[FIRST] + row
        crossed = False
        for u in range(1, start_ref.shape[0]):
            crossed |= (start_ref[u] > position - RIM) & (start_ref[u] < position + ROWS + RIM)

        def run(masked):
            totals = convolve(
                padded, row, weights, 0, weights.shape[0], position, start_ref, end_ref, masked
            )
            for c, total in enumerate(totals):
                out[pl.ds(row, ROWS), c * LANES : (c + 1) * LANES] = total

        pl.when(crossed)(lambda: run(True))
        pl.when(jnp.logical_not(crossed))(lambda: run(False))
        return carry

    lax.fori_loop(0, rows // ROWS, step, 0)


def convolve_inner(me, starts, ends, gated, weights):
    rows, width = gated.shape
    return pl.pallas_call(
        inner_kernel,
        out_shape=jax.ShapeDtypeStruct(gated.shape, jnp.float32),
        in_specs=[SMEM] * 3 + [HBM, VMEM],
        out_specs=VMEM,
        scratch_shapes=[
            pltpu.VMEM((width // LANES, rows + 2 * RIM, LANES), jnp.float32),
            pltpu.VMEM(gated.shape, jnp.bfloat16),
            pltpu.SemaphoreType.DMA((PIECE_COUNT,)),
        ],
        compiler_params=pltpu.CompilerParams(vmem_limit_bytes=60 * 1024 * 1024),
    )(me, starts, ends, gated, weights)


def last_kernel(
    me, start_ref, end_ref, inner, left, right, residual_hbm, weights, gain, w_proj_hbm, out, *scratch
):
    w_proj, residual, total, edge, sems, residual_sems = scratch
    copies = copy_rows(w_proj_hbm, w_proj, sems) + copy_rows(residual_hbm, residual, residual_sems)
    rows, width = inner.shape
    total[...] = inner[...]
    count = weights.shape[0]
    for side, rim in enumerate((left, right)):
        at = 0 if side == 0 else 2 * RIM
        row = 0 if side == 0 else rows - ROWS
        for c in range(width // LANES):
            edge[c] = jnp.zeros(edge.shape[1:], jnp.float32)
            edge[c, at : at + RIM] = rim[:, c * LANES : (c + 1) * LANES].astype(jnp.float32)
        span = (0, RIM - 1) if side == 0 else (RIM, count)
        parts = convolve(
            edge, 0, weights, *span, me[FIRST] + row, start_ref, end_ref, True
        )
        for c, part in enumerate(parts):
            lanes = slice(c * LANES, (c + 1) * LANES)
            total[row : row + ROWS, lanes] = total[row : row + ROWS, lanes] + part
    normed = normalize(total[...], gain[0:1, :])
    activated = (normed * jax.nn.sigmoid(normed)).astype(jnp.bfloat16)
    wait_all(copies)
    projected = jnp.dot(activated, w_proj[...], preferred_element_type=jnp.float32)
    out[...] = (residual[...].astype(jnp.float32) + projected).astype(jnp.bfloat16)


def finish_block(me, starts, ends, inner, left, right, residual, weights, gain, w_proj):
    _, width = inner.shape
    return pl.pallas_call(
        last_kernel,
        out_shape=jax.ShapeDtypeStruct(residual.shape, jnp.bfloat16),
        in_specs=[SMEM] * 3 + [VMEM] * 3 + [HBM] + [VMEM] * 2 + [HBM],
        out_specs=VMEM,
        scratch_shapes=[
            pltpu.VMEM(w_proj.shape, jnp.bfloat16),
            pltpu.VMEM(residual.shape, jnp.bfloat16),
            pltpu.VMEM(inner.shape, jnp.float32),
            pltpu.VMEM((width // LANES, 3 * RIM, LANES), jnp.float32),
            pltpu.SemaphoreType.DMA((PIECE_COUNT,)),
            pltpu.SemaphoreType.DMA((PIECE_COUNT,)),
        ],
        compiler_params=pltpu.CompilerParams(vmem_limit_bytes=58 * 1024 * 1024),
    )(me, starts, ends, inner, left, right, residual, weights, gain, w_proj)


def body(
    frames, utt_lengths, attn_gain, w_qkv, w_out, conv_gain, w_glu, w_depth, depth_gain, w_proj
):
    frame_rows = frames.shape[1]
    block_index = lax.axis_index("blk")
    group_index = lax.axis_index("grp")
    z, yl = block_index // 2, block_index % 2
    x, core = group_index // 4, group_index % 2
    window_start = group_index * (16 * frame_rows)
    first_frame = window_start + block_index * frame_rows
    local_frames = frames[0]
    me = jnp.stack([x, core, z, yl, window_start, first_frame]).astype(jnp.int32)

    shard = w_qkv.T

    def route(offset):
        return lambda x, yh, c, z, yl: (
            (x - offset, yh, yh, z, c) if yl == c else (x - offset, 1 - yh, yh, z, c)
        )

    swap = lambda x, yh, c, z, yl: (x, yh, 1 - c, z, yl)
    across = lambda x, yh, c, z, yl: (x, yh, c, z, 1 - yl)
    near = [send(shard, route(o)) for o in OFFSETS]
    other_frames = send(local_frames, across)
    far = [send(piece, swap) for piece in near]
    key_value, *queries = project_qkv(me, local_frames, other_frames, attn_gain[None, :], near + far)
    groups = [[2 * z + yl for z in range(8)] for yl in range(2)]
    key_value = lax.all_to_all(key_value, "blk", 0, 0, axis_index_groups=groups, tiled=True)
    for d in SEND_ORDER:
        queries[d] = send(queries[d], lambda x, yh, c, z, yl: (x, yh, c, z + d, yl))
    ends = jnp.cumsum(utt_lengths)
    starts = ends - utt_lengths
    mixed = jnp.zeros((16, HEAD, frame_rows), jnp.bfloat16)
    for pieces in PIECES:
        ready = [queries[d] for d in pieces]
        mixed = attend(pieces, me, starts, ends, key_value, mixed, ready)
    mixed = lax.all_to_all(mixed, "blk", 0, 0, tiled=True)
    residual, gated = gate(mixed, local_frames, conv_gain[None, :], w_out, w_glu)

    def neighbour(step):
        def target(x, yh, c, z, yl):
            place = (x * 4 + yh * 2 + c) * 16 + z * 2 + yl + step
            return (place % 16) * 16 + place // 16 if 0 <= place < 256 else None

        return target

    left = send(gated[frame_rows - RIM :], neighbour(1))
    right = send(gated[:RIM], neighbour(-1))
    where = (me, starts, ends)
    inner = convolve_inner(*where, gated, w_depth)
    result = finish_block(*where, inner, left, right, residual, w_depth, depth_gain[None, :], w_proj)
    return result[None]


def solution(mesh):
    in_specs = (P("grp", "blk", None), P(), P(), P(None, "grp"), P(), P(), P(), P(), P(), P())
    out_specs = P("grp", "blk", None)
    return jax.shard_map(body, mesh=mesh, in_specs=in_specs, out_specs=out_specs, check_vma=False)
```

```python
import functools

import jax
import jax.numpy as jnp
from jax import lax
from jax.experimental import pallas as pl
from jax.experimental.pallas import tpu as pltpu
from jax.sharding import PartitionSpec as P


HEAD = 64
LANES = 128
KEY_CHUNK = 512
RIM = 16
ROWS = 16
OFFSETS = (0, 1, 3, 2)
SEND_ORDER = (1, 7, 2, 6, 3, 5, 4)
PIECES = ((0, 1, 7), (2, 6, 3, 5, 4))
LOG2E = 1.4426950408889634

epsilon = 1e-05
big_negative = -1e30


VMEM = pl.BlockSpec(memory_space=pltpu.VMEM)
SMEM = pl.BlockSpec(memory_space=pltpu.SMEM)
HBM = pl.BlockSpec(memory_space=pltpu.HBM)


def coords(index):
    b, g = divmod(index, 16)
    return g // 4, (g // 2) % 2, g % 2, b // 2, b % 2


def flat(x, yh, core, z, yl):
    return ((z % 8) * 2 + yl) * 16 + (x % 4) * 4 + yh * 2 + core


def send(value, target):
    pairs = []
    for source in range(256):
        to = target(*coords(source))
        if to is not None:
            pairs.append((source, to if isinstance(to, int) else flat(*to)))
    return lax.ppermute(value, ("blk", "grp"), pairs)


def normalize(values, row_gain):
    center = values - jnp.mean(values, axis=-1, keepdims=True)
    spread = jnp.mean(center * center, axis=-1, keepdims=True)
    return center * lax.rsqrt(spread + epsilon) * row_gain


def low_lanes(rows):
    return lax.broadcasted_iota(jnp.int32, (rows, LANES), 1) < HEAD


def swap_lanes(values):
    return pltpu.roll(values, HEAD, 1)


X, CORE, Z, YL, WINDOW, FIRST = range(6)


def shard_head(me, i):
    core = me[CORE] if i < 4 else 1 - me[CORE]
    return 2 * lax.rem(me[X] + OFFSETS[i % 4], 4) + core


def inside(position, start_ref, end_ref, place):
    start, end = jnp.zeros_like(position), jnp.zeros_like(position)
    for u in range(start_ref.shape[0]):
        start, end = jnp.where(place == u, start_ref[u], start), jnp.where(place == u, end_ref[u], end)
    return (position >= start) & (position < end)


CONTRACT = (((1,), (1,)), ((), ()))


def transposed(out, index, start, flipped):
    for j in range(flipped.shape[1] // LANES):
        at = start + j * HEAD
        out[index, at : at + HEAD] = flipped[:, j * LANES : (j + 1) * LANES].astype(jnp.bfloat16)


def norm_kernel(frames, gain, out):
    out[...] = normalize(frames[...].astype(jnp.float32), gain[0:1, :]).astype(jnp.bfloat16)


def norm(frames, gain):
    return pl.pallas_call(
        norm_kernel,
        out_shape=jax.ShapeDtypeStruct(frames.shape, jnp.bfloat16),
        in_specs=[VMEM] * 2,
        out_specs=VMEM,
        compiler_params=pltpu.CompilerParams(vmem_limit_bytes=8 * 1024 * 1024),
    )(frames, gain)


def key_value_kernel(me, own, other, *refs):
    shards, out, both_rows = refs[:8], refs[8], refs[9]
    rows = own.shape[0]
    both_rows[:rows] = own[...]
    both_rows[rows:] = other[...]
    low = low_lanes(rows)
    for i in range(0, 8, 2):
        heads = shard_head(me, i), shard_head(me, i + 1)
        weights = jnp.concatenate([shards[j][HEAD : 2 * HEAD, :] for j in (i, i + 1)], axis=0)
        both = lax.dot_general(both_rows[...], weights, CONTRACT, preferred_element_type=jnp.float32)
        mine, theirs = both[:rows], both[rows:]
        out[heads[0], :rows] = jnp.where(low, mine, swap_lanes(theirs)).astype(jnp.bfloat16)
        out[heads[1], :rows] = jnp.where(low, swap_lanes(mine), theirs).astype(jnp.bfloat16)
        weights = jnp.concatenate([shards[j][2 * HEAD :, :] for j in (i, i + 1)], axis=0)
        both = lax.dot_general(weights, both_rows[...], CONTRACT, preferred_element_type=jnp.float32)
        transposed(out, heads[0], rows, both[:HEAD])
        transposed(out, heads[1], rows, both[HEAD:])


def query_kernel(me, own, other, *refs):
    shards, pieces, both_rows, staged = refs[:8], refs[8:16], refs[16], refs[17]
    rows = own.shape[0]
    both_rows[:rows] = own[...]
    both_rows[rows:] = other[...]
    for i in range(0, 8, 2):
        weights = jnp.concatenate([shards[j][:HEAD, :] for j in (i, i + 1)], axis=0)
        both = lax.dot_general(weights, both_rows[...], CONTRACT, preferred_element_type=jnp.float32)
        both = both * (HEAD**-0.5 * LOG2E)
        for j in range(2):
            piece = lax.rem(shard_head(me, i + j) + 8 - me[Z], 8)
            transposed(staged, piece, 0, both[j * HEAD : (j + 1) * HEAD])
    for d in range(8):
        pieces[d][...] = staged[d]


def project(kernel, shapes, staged, me, own, other, shards):
    rows, width = own.shape
    return pl.pallas_call(
        kernel,
        out_shape=[jax.ShapeDtypeStruct(shape, jnp.bfloat16) for shape in shapes],
        in_specs=[SMEM] + [VMEM] * 10,
        out_specs=[VMEM] * len(shapes),
        scratch_shapes=[pltpu.VMEM((2 * rows, width), jnp.bfloat16)]
        + [pltpu.VMEM(shape, jnp.bfloat16) for shape in staged],
        compiler_params=pltpu.CompilerParams(vmem_limit_bytes=16 * 1024 * 1024),
    )(me, own, other, *shards)


def attend_kernel(pieces, me, start_ref, end_ref, in_ref, before, *refs):
    count = len(pieces)
    parts_hbm, out_ref = refs[:count], refs[count]
    keys, values, queries, scores, most_ref, parts_q, sems = refs[count + 1 :]
    copies = [pltpu.make_async_copy(parts_hbm[d], parts_q.at[d], sems.at[d]) for d in range(count)]
    for copy in copies:
        copy.start()
    out_ref[...] = before[...]
    sources = in_ref.shape[0]
    block = in_ref.shape[1] // 2
    low = low_lanes(block)
    row = lax.broadcasted_iota(jnp.int32, (block, LANES), 0)
    lane = lax.broadcasted_iota(jnp.int32, (block, LANES), 1) - HEAD
    place = lax.broadcasted_iota(jnp.int32, (16, block), 0)
    column = lax.broadcasted_iota(jnp.int32, (16, block), 1)
    window = keys.shape[0]
    top = lax.broadcasted_iota(jnp.int32, (values.shape[1] - HEAD, KEY_CHUNK), 0) == 0
    for j in range(values.shape[0]):
        values[j, HEAD:] = jnp.where(top, 1.0, 0.0).astype(jnp.bfloat16)

    def prepare(s, carry):
        key = in_ref[s, :block].astype(jnp.float32)
        for side in range(2):
            shard = 2 * s + (me[YL] if side == 0 else 1 - me[YL])
            base = me[WINDOW] + shard * block
            at = pl.ds(pl.multiple_of((2 * s + side) * block, block), block)
            mask = jnp.where(inside(row + base, start_ref, end_ref, lane), 0.0, big_negative)
            keys[at, :] = jnp.where(low, swap_lanes(key) if side else key, mask).astype(jnp.bfloat16)
        for i in range(2 * block // LANES):
            at = block + i * HEAD
            values[s, :HEAD, i * LANES : (i + 1) * LANES] = in_ref[s, at : at + HEAD]
        return carry

    def origin(i):
        side, d = lax.rem(i, 2), pieces[0]
        for j in range(1, count):
            d = jnp.where(i // 2 == j, pieces[j], d)
        shard = jnp.where(side == 0, me[YL], 1 - me[YL])
        return 2 * lax.rem(me[Z] + 8 - d, 8) + shard

    for i in range(2 * count):
        if i % 2 == 0:
            copies[i // 2].wait()
        mark = inside(column + (me[WINDOW] + origin(i) * block), start_ref, end_ref, place)
        queries[i, HEAD : HEAD + 16] = jnp.where(mark, 1.0, 0.0).astype(jnp.bfloat16)
        queries[i, HEAD + 16 :] = jnp.zeros((HEAD - 16, block), jnp.bfloat16)
        for j in range(block // LANES):
            at = ((i % 2) * (block // LANES) + j) * HEAD
            queries[i, :HEAD, j * LANES : (j + 1) * LANES] = parts_q[i // 2, at : at + HEAD]
    lax.fori_loop(0, sources, prepare, 0)
    chunks = window // KEY_CHUNK

    def score(query, j):
        at = slice(j * KEY_CHUNK, (j + 1) * KEY_CHUNK)
        return jnp.dot(keys[at, :], query, preferred_element_type=jnp.float32)

    def weigh(j, most):
        probs = jnp.exp2(scores[j * KEY_CHUNK : (j + 1) * KEY_CHUNK, :] - most)
        return jnp.dot(values[j], probs.astype(jnp.bfloat16), preferred_element_type=jnp.float32)

    def finish(total, i):
        mixed = total[:HEAD] / total[HEAD : HEAD + 1]
        out_ref[origin(i)] = mixed.astype(jnp.bfloat16)

    def step(i, carry):
        query = queries[i]
        most = most_ref[0:1, :]
        best, total = None, None
        for j in range(chunks):
            part = weigh(j, most)
            total = part if total is None else total + part
            part = score(query, j)
            scores[j * KEY_CHUNK : (j + 1) * KEY_CHUNK, :] = part
            part = jnp.max(part.reshape(KEY_CHUNK // 8, 8, block), axis=0)
            best = part if best is None else jnp.maximum(best, part)
        most_ref[...] = jnp.broadcast_to(jnp.max(best, axis=0, keepdims=True), (8, block))
        finish(total, jnp.maximum(i - 1, 0))
        return carry

    lax.fori_loop(0, 2 * count, step, 0)
    total = None
    for j in range(chunks):
        part = weigh(j, most_ref[0:1, :])
        total = part if total is None else total + part
    finish(total, 2 * count - 1)


def attend(pieces, me, starts, ends, key_value, before, queries):
    sources, block = key_value.shape[0], key_value.shape[1] // 2
    window, count = 2 * block * sources, len(pieces)
    return pl.pallas_call(
        functools.partial(attend_kernel, pieces),
        out_shape=jax.ShapeDtypeStruct((2 * sources, HEAD, block), jnp.bfloat16),
        in_specs=[SMEM] * 3 + [VMEM] * 2 + [HBM] * count,
        out_specs=VMEM,
        scratch_shapes=[
            pltpu.VMEM((window, LANES), jnp.bfloat16),
            pltpu.VMEM((window // KEY_CHUNK, HEAD + 16, KEY_CHUNK), jnp.bfloat16),
            pltpu.VMEM((2 * count, LANES, block), jnp.bfloat16),
            pltpu.VMEM((window, block), jnp.float32),
            pltpu.VMEM((8, block), jnp.float32),
            pltpu.VMEM((count, block, LANES), jnp.bfloat16),
            pltpu.SemaphoreType.DMA((count,)),
        ],
        compiler_params=pltpu.CompilerParams(vmem_limit_bytes=24 * 1024 * 1024),
    )(me, starts, ends, key_value, before, *queries)


def gate_kernel(mixed, frames, gain, w_out_hbm, w_glu_hbm, residual_ref, gated_ref, *scratch):
    w_out, w_glu, attended, out_sem, glu_sem = scratch
    out_copy = pltpu.make_async_copy(w_out_hbm, w_out, out_sem)
    glu_copy = pltpu.make_async_copy(w_glu_hbm, w_glu, glu_sem)
    out_copy.start()
    glu_copy.start()
    heads = mixed.shape[0]
    for pair in range(heads // 2):
        flipped = jnp.concatenate([mixed[2 * pair], mixed[2 * pair + 1]], axis=0).astype(jnp.float32)
        attended[:, pair * LANES : (pair + 1) * LANES] = flipped.T.astype(jnp.bfloat16)
    out_copy.wait()
    projected = jnp.dot(attended[...], w_out[...], preferred_element_type=jnp.float32)
    residual = (frames[...].astype(jnp.float32) + projected).astype(jnp.bfloat16)
    residual_ref[...] = residual
    width = frames.shape[1]
    conv_in = normalize(residual.astype(jnp.float32), gain[0:1, :]).astype(jnp.bfloat16)
    glu_copy.wait()
    step = 256
    for j in range(0, width, step):
        a = jnp.dot(conv_in, w_glu[:, j : j + step], preferred_element_type=jnp.float32)
        b = jnp.dot(conv_in, w_glu[:, width + j : width + j + step], preferred_element_type=jnp.float32)
        gated_ref[:, j : j + step] = (a * jax.nn.sigmoid(b)).astype(jnp.bfloat16)


def gate(mixed, frames, gain, w_out, w_glu):
    shape = jax.ShapeDtypeStruct(frames.shape, jnp.bfloat16)
    return pl.pallas_call(
        gate_kernel,
        out_shape=[shape, shape],
        in_specs=[VMEM] * 3 + [HBM] * 2,
        out_specs=[VMEM] * 2,
        scratch_shapes=[
            pltpu.VMEM(w_out.shape, jnp.bfloat16),
            pltpu.VMEM(w_glu.shape, jnp.bfloat16),
            pltpu.VMEM(frames.shape, jnp.bfloat16),
            pltpu.SemaphoreType.DMA,
            pltpu.SemaphoreType.DMA,
        ],
        compiler_params=pltpu.CompilerParams(vmem_limit_bytes=24 * 1024 * 1024),
    )(mixed, frames, gain, w_out, w_glu)


def convolve(source, row, weights, t_first, t_last, position, start_ref, end_ref, masked):
    place = lax.broadcasted_iota(jnp.int32, (ROWS, LANES), 0) + position
    lo, hi = jnp.zeros_like(place), jnp.zeros_like(place)
    if masked:
        for u in range(start_ref.shape[0]):
            inside = (place >= start_ref[u]) & (place < end_ref[u])
            lo, hi = jnp.where(inside, start_ref[u], lo), jnp.where(inside, end_ref[u], hi)
        lo, hi = lo - place, hi - place
    tiles = source.shape[0]
    totals = [None] * tiles
    for t in range(t_first, t_last):
        same = (lo <= t - RIM + 1) & (hi > t - RIM + 1) if masked else None
        for c in range(tiles):
            term = source[c, pl.ds(row + t + 1, ROWS), :] * weights[t : t + 1, c * LANES : (c + 1) * LANES]
            term = jnp.where(same, term, 0.0) if masked else term
            totals[c] = term if totals[c] is None else totals[c] + term
    return totals


def inner_kernel(me, start_ref, end_ref, gated, weights, out, padded):
    rows, width = gated.shape
    for c in range(width // LANES):
        padded[c, :RIM] = jnp.zeros((RIM, LANES), jnp.float32)
        padded[c, RIM : RIM + rows] = gated[:, c * LANES : (c + 1) * LANES].astype(jnp.float32)
        padded[c, RIM + rows :] = jnp.zeros((RIM, LANES), jnp.float32)

    def step(i, carry):
        row = pl.multiple_of(i * ROWS, ROWS)
        position = me[FIRST] + row
        crossed = False
        for u in range(1, start_ref.shape[0]):
            crossed |= (start_ref[u] > position - RIM) & (start_ref[u] < position + ROWS + RIM)

        def run(masked):
            totals = convolve(
                padded, row, weights, 0, weights.shape[0], position, start_ref, end_ref, masked
            )
            for c, total in enumerate(totals):
                out[pl.ds(row, ROWS), c * LANES : (c + 1) * LANES] = total

        pl.when(crossed)(lambda: run(True))
        pl.when(jnp.logical_not(crossed))(lambda: run(False))
        return carry

    lax.fori_loop(0, rows // ROWS, step, 0)


def convolve_inner(me, starts, ends, gated, weights):
    rows, width = gated.shape
    return pl.pallas_call(
        inner_kernel,
        out_shape=jax.ShapeDtypeStruct(gated.shape, jnp.float32),
        in_specs=[SMEM] * 3 + [VMEM] * 2,
        out_specs=VMEM,
        scratch_shapes=[pltpu.VMEM((width // LANES, rows + 2 * RIM, LANES), jnp.float32)],
        compiler_params=pltpu.CompilerParams(vmem_limit_bytes=16 * 1024 * 1024),
    )(me, starts, ends, gated, weights)


def last_kernel(
    me, start_ref, end_ref, inner, left, right, residual, weights, gain, w_proj_hbm, out, *scratch
):
    w_proj, total, edge, sem = scratch
    copy = pltpu.make_async_copy(w_proj_hbm, w_proj, sem)
    copy.start()
    rows, width = inner.shape
    total[...] = inner[...]
    count = weights.shape[0]
    for side, rim in enumerate((left, right)):
        at = 0 if side == 0 else 2 * RIM
        row = 0 if side == 0 else rows - ROWS
        for c in range(width // LANES):
            edge[c] = jnp.zeros(edge.shape[1:], jnp.float32)
            edge[c, at : at + RIM] = rim[:, c * LANES : (c + 1) * LANES].astype(jnp.float32)
        span = (0, RIM - 1) if side == 0 else (RIM, count)
        parts = convolve(
            edge, 0, weights, *span, me[FIRST] + row, start_ref, end_ref, True
        )
        for c, part in enumerate(parts):
            lanes = slice(c * LANES, (c + 1) * LANES)
            total[row : row + ROWS, lanes] = total[row : row + ROWS, lanes] + part
    normed = normalize(total[...], gain[0:1, :])
    activated = (normed * jax.nn.sigmoid(normed)).astype(jnp.bfloat16)
    copy.wait()
    projected = jnp.dot(activated, w_proj[...], preferred_element_type=jnp.float32)
    out[...] = (residual[...].astype(jnp.float32) + projected).astype(jnp.bfloat16)


def finish_block(me, starts, ends, inner, left, right, residual, weights, gain, w_proj):
    _, width = inner.shape
    return pl.pallas_call(
        last_kernel,
        out_shape=jax.ShapeDtypeStruct(residual.shape, jnp.bfloat16),
        in_specs=[SMEM] * 3 + [VMEM] * 6 + [HBM],
        out_specs=VMEM,
        scratch_shapes=[
            pltpu.VMEM(w_proj.shape, jnp.bfloat16),
            pltpu.VMEM(inner.shape, jnp.float32),
            pltpu.VMEM((width // LANES, 3 * RIM, LANES), jnp.float32),
            pltpu.SemaphoreType.DMA,
        ],
        compiler_params=pltpu.CompilerParams(vmem_limit_bytes=24 * 1024 * 1024),
    )(me, starts, ends, inner, left, right, residual, weights, gain, w_proj)


def body(
    frames, utt_lengths, attn_gain, w_qkv, w_out, conv_gain, w_glu, w_depth, depth_gain, w_proj
):
    frame_rows = frames.shape[1]
    block_index = lax.axis_index("blk")
    group_index = lax.axis_index("grp")
    z, yl = block_index // 2, block_index % 2
    x, core = group_index // 4, group_index % 2
    window_start = group_index * (16 * frame_rows)
    first_frame = window_start + block_index * frame_rows
    local_frames = frames[0]
    me = jnp.stack([x, core, z, yl, window_start, first_frame]).astype(jnp.int32)

    shard = w_qkv.T

    def route(offset):
        return lambda x, yh, c, z, yl: (
            (x - offset, yh, yh, z, c) if yl == c else (x - offset, 1 - yh, yh, z, c)
        )

    swap = lambda x, yh, c, z, yl: (x, yh, 1 - c, z, yl)
    across = lambda x, yh, c, z, yl: (x, yh, c, z, 1 - yl)
    near = [send(shard, route(o)) for o in OFFSETS]
    own = norm(local_frames, attn_gain[None, :])
    other = send(own, across)
    far = [send(piece, swap) for piece in near]
    stream = (me, own, other, near + far)
    (key_value,) = project(key_value_kernel, [(8, 2 * frame_rows, LANES)], [], *stream)
    piece = (frame_rows, LANES)
    queries = project(query_kernel, [piece] * 8, [(8,) + piece], *stream)
    groups = [[2 * z + yl for z in range(8)] for yl in range(2)]
    key_value = lax.all_to_all(key_value, "blk", 0, 0, axis_index_groups=groups, tiled=True)
    queries = list(queries)
    for d in SEND_ORDER:
        queries[d] = send(queries[d], lambda x, yh, c, z, yl: (x, yh, c, z + d, yl))
    ends = jnp.cumsum(utt_lengths)
    starts = ends - utt_lengths
    mixed = jnp.zeros((16, HEAD, frame_rows), jnp.bfloat16)
    for pieces in PIECES:
        ready = [queries[d] for d in pieces]
        mixed = attend(pieces, me, starts, ends, key_value, mixed, ready)
    mixed = lax.all_to_all(mixed, "blk", 0, 0, tiled=True)
    residual, gated = gate(mixed, local_frames, conv_gain[None, :], w_out, w_glu)

    def neighbour(step):
        def target(x, yh, c, z, yl):
            place = (x * 4 + yh * 2 + c) * 16 + z * 2 + yl + step
            return (place % 16) * 16 + place // 16 if 0 <= place < 256 else None

        return target

    left = send(gated[frame_rows - RIM :], neighbour(1))
    right = send(gated[:RIM], neighbour(-1))
    where = (me, starts, ends)
    inner = convolve_inner(*where, gated, w_depth)
    result = finish_block(*where, inner, left, right, residual, w_depth, depth_gain[None, :], w_proj)
    return result[None]


def solution(mesh):
    in_specs = (P("grp", "blk", None), P(), P(), P(None, "grp"), P(), P(), P(), P(), P(), P())
    out_specs = P("grp", "blk", None)
    return jax.shard_map(body, mesh=mesh, in_specs=in_specs, out_specs=out_specs, check_vma=False)
```

```python
import functools

import jax
import jax.numpy as jnp
from jax import lax
from jax.experimental import pallas as pl
from jax.experimental.pallas import tpu as pltpu
from jax.sharding import PartitionSpec as P


HEAD = 64
LANES = 128
KEY_CHUNK = 512
RIM = 16
ROWS = 16
OFFSETS = (0, 1, 3, 2)
SEND_ORDER = (1, 7, 2, 6, 3, 5, 4)
PIECES = ((0, 1, 7), (2, 6, 3, 5, 4))
LOG2E = 1.4426950408889634

epsilon = 1e-05
big_negative = -1e30


VMEM = pl.BlockSpec(memory_space=pltpu.VMEM)
SMEM = pl.BlockSpec(memory_space=pltpu.SMEM)
HBM = pl.BlockSpec(memory_space=pltpu.HBM)


def coords(index):
    b, g = divmod(index, 16)
    return g // 4, (g // 2) % 2, g % 2, b // 2, b % 2


def flat(x, yh, core, z, yl):
    return ((z % 8) * 2 + yl) * 16 + (x % 4) * 4 + yh * 2 + core


def send(value, target):
    pairs = []
    for source in range(256):
        to = target(*coords(source))
        if to is not None:
            pairs.append((source, to if isinstance(to, int) else flat(*to)))
    return lax.ppermute(value, ("blk", "grp"), pairs)


def normalize(values, row_gain):
    center = values - jnp.mean(values, axis=-1, keepdims=True)
    spread = jnp.mean(center * center, axis=-1, keepdims=True)
    return center * lax.rsqrt(spread + epsilon) * row_gain


def low_lanes(rows):
    return lax.broadcasted_iota(jnp.int32, (rows, LANES), 1) < HEAD


def swap_lanes(values):
    return pltpu.roll(values, HEAD, 1)


X, CORE, Z, YL, WINDOW, FIRST = range(6)


def shard_head(me, i):
    core = me[CORE] if i < 4 else 1 - me[CORE]
    return 2 * lax.rem(me[X] + OFFSETS[i % 4], 4) + core


def inside(position, start_ref, end_ref, place):
    start, end = jnp.zeros_like(position), jnp.zeros_like(position)
    for u in range(start_ref.shape[0]):
        start, end = jnp.where(place == u, start_ref[u], start), jnp.where(place == u, end_ref[u], end)
    return (position >= start) & (position < end)


CONTRACT = (((1,), (1,)), ((), ()))


def transposed(out, index, start, flipped):
    for j in range(flipped.shape[1] // LANES):
        at = start + j * HEAD
        out[index, at : at + HEAD] = flipped[:, j * LANES : (j + 1) * LANES].astype(jnp.bfloat16)


def norm_kernel(frames, gain, out):
    out[...] = normalize(frames[...].astype(jnp.float32), gain[0:1, :]).astype(jnp.bfloat16)


def norm(frames, gain):
    return pl.pallas_call(
        norm_kernel,
        out_shape=jax.ShapeDtypeStruct(frames.shape, jnp.bfloat16),
        in_specs=[VMEM] * 2,
        out_specs=VMEM,
        compiler_params=pltpu.CompilerParams(vmem_limit_bytes=8 * 1024 * 1024),
    )(frames, gain)


def key_value_kernel(me, own, other, *refs):
    near, far_hbm, out_hbm, stream, far, out, sems, out_sems = refs[:4], refs[4:8], *refs[8:]
    copies = [pltpu.make_async_copy(far_hbm[i], far.at[i], sems.at[i]) for i in range(4)]
    for copy in copies:
        copy.start()
    rows = own.shape[0]
    stream[:rows] = own[...]
    stream[rows:] = other[...]
    low = low_lanes(rows)
    leaving = []
    for first, part in ((0, near), (4, [far.at[i] for i in range(4)])):
        if first:
            for copy in copies:
                copy.wait()
        heads = [shard_head(me, first + j) for j in range(4)]
        weights = jnp.concatenate([shard[HEAD : 2 * HEAD, :] for shard in part], axis=0)
        both = lax.dot_general(stream[...], weights, CONTRACT, preferred_element_type=jnp.float32)
        for j in (0, 2):
            pair = both[:, j * HEAD : (j + 2) * HEAD]
            mine, theirs = pair[:rows], pair[rows:]
            out[first + j, :rows] = jnp.where(low, mine, swap_lanes(theirs)).astype(jnp.bfloat16)
            out[first + j + 1, :rows] = jnp.where(low, swap_lanes(mine), theirs).astype(jnp.bfloat16)
        weights = jnp.concatenate([shard[2 * HEAD :, :] for shard in part], axis=0)
        both = lax.dot_general(weights, stream[...], CONTRACT, preferred_element_type=jnp.float32)
        for j in range(4):
            i = first + j
            transposed(out, i, rows, both[j * HEAD : (j + 1) * HEAD])
            leaving.append(pltpu.make_async_copy(out.at[i], out_hbm.at[heads[j]], out_sems.at[i]))
            leaving[-1].start()
    for copy in leaving:
        copy.wait()


def project_key_value(me, own, other, shards):
    rows, width = own.shape
    shape = (8, 2 * rows, LANES)
    return pl.pallas_call(
        key_value_kernel,
        out_shape=jax.ShapeDtypeStruct(shape, jnp.bfloat16),
        in_specs=[SMEM] + [VMEM] * 6 + [HBM] * 4,
        out_specs=HBM,
        scratch_shapes=[
            pltpu.VMEM((2 * rows, width), jnp.bfloat16),
            pltpu.VMEM((4,) + shards[0].shape, jnp.bfloat16),
            pltpu.VMEM(shape, jnp.bfloat16),
            pltpu.SemaphoreType.DMA((4,)),
            pltpu.SemaphoreType.DMA((8,)),
        ],
        compiler_params=pltpu.CompilerParams(vmem_limit_bytes=16 * 1024 * 1024),
    )(me, own, other, *shards)


def query_kernel(me, own, other, *refs):
    shards, pieces, both_rows, staged = refs[:8], refs[8:16], refs[16], refs[17]
    rows = own.shape[0]
    both_rows[:rows] = own[...]
    both_rows[rows:] = other[...]
    weights = jnp.concatenate([shard[:HEAD, :] for shard in shards], axis=0)
    both = lax.dot_general(weights, both_rows[...], CONTRACT, preferred_element_type=jnp.float32)
    both = both * (HEAD**-0.5 * LOG2E)
    for i in range(8):
        piece = lax.rem(shard_head(me, i) + 8 - me[Z], 8)
        transposed(staged, piece, 0, both[i * HEAD : (i + 1) * HEAD])
    for d in range(8):
        pieces[d][...] = staged[d]


def project(kernel, shapes, staged, me, own, other, shards):
    rows, width = own.shape
    return pl.pallas_call(
        kernel,
        out_shape=[jax.ShapeDtypeStruct(shape, jnp.bfloat16) for shape in shapes],
        in_specs=[SMEM] + [VMEM] * 10,
        out_specs=[VMEM] * len(shapes),
        scratch_shapes=[pltpu.VMEM((2 * rows, width), jnp.bfloat16)]
        + [pltpu.VMEM(shape, jnp.bfloat16) for shape in staged],
        compiler_params=pltpu.CompilerParams(vmem_limit_bytes=16 * 1024 * 1024),
    )(me, own, other, *shards)


def attend_kernel(pieces, me, start_ref, end_ref, in_ref, before, *refs):
    count = len(pieces)
    parts_hbm, out_ref = refs[:count], refs[count]
    keys, values, queries, scores, most_ref, parts_q, sems = refs[count + 1 :]
    copies = [pltpu.make_async_copy(parts_hbm[d], parts_q.at[d], sems.at[d]) for d in range(count)]
    for copy in copies:
        copy.start()
    out_ref[...] = before[...]
    sources = in_ref.shape[0]
    block = in_ref.shape[1] // 2
    low = low_lanes(block)
    row = lax.broadcasted_iota(jnp.int32, (block, LANES), 0)
    lane = lax.broadcasted_iota(jnp.int32, (block, LANES), 1) - HEAD
    place = lax.broadcasted_iota(jnp.int32, (16, block), 0)
    column = lax.broadcasted_iota(jnp.int32, (16, block), 1)
    window = keys.shape[0]
    top = lax.broadcasted_iota(jnp.int32, (values.shape[1] - HEAD, KEY_CHUNK), 0) == 0
    for j in range(values.shape[0]):
        values[j, HEAD:] = jnp.where(top, 1.0, 0.0).astype(jnp.bfloat16)

    def prepare(s, carry):
        key = in_ref[s, :block].astype(jnp.float32)
        for side in range(2):
            shard = 2 * s + (me[YL] if side == 0 else 1 - me[YL])
            base = me[WINDOW] + shard * block
            at = pl.ds(pl.multiple_of((2 * s + side) * block, block), block)
            mask = jnp.where(inside(row + base, start_ref, end_ref, lane), 0.0, big_negative)
            keys[at, :] = jnp.where(low, swap_lanes(key) if side else key, mask).astype(jnp.bfloat16)
        for i in range(2 * block // LANES):
            at = block + i * HEAD
            values[s, :HEAD, i * LANES : (i + 1) * LANES] = in_ref[s, at : at + HEAD]
        return carry

    def origin(i):
        side, d = lax.rem(i, 2), pieces[0]
        for j in range(1, count):
            d = jnp.where(i // 2 == j, pieces[j], d)
        shard = jnp.where(side == 0, me[YL], 1 - me[YL])
        return 2 * lax.rem(me[Z] + 8 - d, 8) + shard

    for i in range(2 * count):
        if i % 2 == 0:
            copies[i // 2].wait()
        mark = inside(column + (me[WINDOW] + origin(i) * block), start_ref, end_ref, place)
        queries[i, HEAD : HEAD + 16] = jnp.where(mark, 1.0, 0.0).astype(jnp.bfloat16)
        queries[i, HEAD + 16 :] = jnp.zeros((HEAD - 16, block), jnp.bfloat16)
        for j in range(block // LANES):
            at = ((i % 2) * (block // LANES) + j) * HEAD
            queries[i, :HEAD, j * LANES : (j + 1) * LANES] = parts_q[i // 2, at : at + HEAD]
    lax.fori_loop(0, sources, prepare, 0)
    chunks = window // KEY_CHUNK

    def score(query, j):
        at = slice(j * KEY_CHUNK, (j + 1) * KEY_CHUNK)
        return jnp.dot(keys[at, :], query, preferred_element_type=jnp.float32)

    def weigh(j, most):
        probs = jnp.exp2(scores[j * KEY_CHUNK : (j + 1) * KEY_CHUNK, :] - most)
        return jnp.dot(values[j], probs.astype(jnp.bfloat16), preferred_element_type=jnp.float32)

    def finish(total, i):
        mixed = total[:HEAD] / total[HEAD : HEAD + 1]
        out_ref[origin(i)] = mixed.astype(jnp.bfloat16)

    def keep(j, part, best):
        scores[j * KEY_CHUNK : (j + 1) * KEY_CHUNK, :] = part
        part = jnp.max(part.reshape(KEY_CHUNK // 8, 8, block), axis=0)
        return part if best is None else jnp.maximum(best, part)

    def settle(best):
        most_ref[...] = jnp.broadcast_to(jnp.max(best, axis=0, keepdims=True), (8, block))

    best = None
    for j in range(chunks):
        best = keep(j, score(queries[0], j), best)
    settle(best)

    def step(i, carry):
        query = queries[i]
        most = most_ref[0:1, :]
        best, total = None, None
        for j in range(chunks):
            part = weigh(j, most)
            total = part if total is None else total + part
            best = keep(j, score(query, j), best)
        settle(best)
        finish(total, i - 1)
        return carry

    lax.fori_loop(1, 2 * count, step, 0)
    total = None
    for j in range(chunks):
        part = weigh(j, most_ref[0:1, :])
        total = part if total is None else total + part
    finish(total, 2 * count - 1)


def attend(pieces, me, starts, ends, key_value, before, queries):
    sources, block = key_value.shape[0], key_value.shape[1] // 2
    window, count = 2 * block * sources, len(pieces)
    return pl.pallas_call(
        functools.partial(attend_kernel, pieces),
        out_shape=jax.ShapeDtypeStruct((2 * sources, HEAD, block), jnp.bfloat16),
        in_specs=[SMEM] * 3 + [VMEM] * 2 + [HBM] * count,
        out_specs=VMEM,
        scratch_shapes=[
            pltpu.VMEM((window, LANES), jnp.bfloat16),
            pltpu.VMEM((window // KEY_CHUNK, HEAD + 16, KEY_CHUNK), jnp.bfloat16),
            pltpu.VMEM((2 * count, LANES, block), jnp.bfloat16),
            pltpu.VMEM((window, block), jnp.float32),
            pltpu.VMEM((8, block), jnp.float32),
            pltpu.VMEM((count, block, LANES), jnp.bfloat16),
            pltpu.SemaphoreType.DMA((count,)),
        ],
        compiler_params=pltpu.CompilerParams(vmem_limit_bytes=24 * 1024 * 1024),
    )(me, starts, ends, key_value, before, *queries)


def gate_kernel(mixed, frames, gain, w_out_hbm, w_glu_hbm, residual_ref, gated_ref, *scratch):
    w_out, w_glu, attended, out_sem, glu_sem = scratch
    out_copy = pltpu.make_async_copy(w_out_hbm, w_out, out_sem)
    glu_copy = pltpu.make_async_copy(w_glu_hbm, w_glu, glu_sem)
    out_copy.start()
    glu_copy.start()
    heads = mixed.shape[0]
    for pair in range(heads // 2):
        flipped = jnp.concatenate([mixed[2 * pair], mixed[2 * pair + 1]], axis=0).astype(jnp.float32)
        attended[:, pair * LANES : (pair + 1) * LANES] = flipped.T.astype(jnp.bfloat16)
    out_copy.wait()
    projected = jnp.dot(attended[...], w_out[...], preferred_element_type=jnp.float32)
    residual = (frames[...].astype(jnp.float32) + projected).astype(jnp.bfloat16)
    residual_ref[...] = residual
    width = frames.shape[1]
    conv_in = normalize(residual.astype(jnp.float32), gain[0:1, :]).astype(jnp.bfloat16)
    glu_copy.wait()
    step = 256
    for j in range(0, width, step):
        a = jnp.dot(conv_in, w_glu[:, j : j + step], preferred_element_type=jnp.float32)
        b = jnp.dot(conv_in, w_glu[:, width + j : width + j + step], preferred_element_type=jnp.float32)
        gated_ref[:, j : j + step] = (a * jax.nn.sigmoid(b)).astype(jnp.bfloat16)


def gate(mixed, frames, gain, w_out, w_glu):
    shape = jax.ShapeDtypeStruct(frames.shape, jnp.bfloat16)
    return pl.pallas_call(
        gate_kernel,
        out_shape=[shape, shape],
        in_specs=[VMEM] * 3 + [HBM] * 2,
        out_specs=[VMEM] * 2,
        scratch_shapes=[
            pltpu.VMEM(w_out.shape, jnp.bfloat16),
            pltpu.VMEM(w_glu.shape, jnp.bfloat16),
            pltpu.VMEM(frames.shape, jnp.bfloat16),
            pltpu.SemaphoreType.DMA,
            pltpu.SemaphoreType.DMA,
        ],
        compiler_params=pltpu.CompilerParams(vmem_limit_bytes=24 * 1024 * 1024),
    )(mixed, frames, gain, w_out, w_glu)


def convolve(source, row, weights, t_first, t_last, position, start_ref, end_ref, masked):
    place = lax.broadcasted_iota(jnp.int32, (ROWS, LANES), 0) + position
    lo, hi = jnp.zeros_like(place), jnp.zeros_like(place)
    if masked:
        for u in range(start_ref.shape[0]):
            inside = (place >= start_ref[u]) & (place < end_ref[u])
            lo, hi = jnp.where(inside, start_ref[u], lo), jnp.where(inside, end_ref[u], hi)
        lo, hi = lo - place, hi - place
    tiles = source.shape[0]
    totals = [None] * tiles
    for t in range(t_first, t_last):
        same = (lo <= t - RIM + 1) & (hi > t - RIM + 1) if masked else None
        for c in range(tiles):
            term = source[c, pl.ds(row + t + 1, ROWS), :] * weights[t : t + 1, c * LANES : (c + 1) * LANES]
            term = jnp.where(same, term, 0.0) if masked else term
            totals[c] = term if totals[c] is None else totals[c] + term
    return totals


def inner_kernel(me, start_ref, end_ref, gated, weights, out, padded):
    rows, width = gated.shape
    for c in range(width // LANES):
        padded[c, :RIM] = jnp.zeros((RIM, LANES), jnp.float32)
        padded[c, RIM : RIM + rows] = gated[:, c * LANES : (c + 1) * LANES].astype(jnp.float32)
        padded[c, RIM + rows :] = jnp.zeros((RIM, LANES), jnp.float32)

    def step(i, carry):
        row = pl.multiple_of(i * ROWS, ROWS)
        position = me[FIRST] + row
        crossed = False
        for u in range(1, start_ref.shape[0]):
            crossed |= (start_ref[u] > position - RIM) & (start_ref[u] < position + ROWS + RIM)

        def run(masked):
            totals = convolve(
                padded, row, weights, 0, weights.shape[0], position, start_ref, end_ref, masked
            )
            for c, total in enumerate(totals):
                out[pl.ds(row, ROWS), c * LANES : (c + 1) * LANES] = total

        pl.when(crossed)(lambda: run(True))
        pl.when(jnp.logical_not(crossed))(lambda: run(False))
        return carry

    lax.fori_loop(0, rows // ROWS, step, 0)


def convolve_inner(me, starts, ends, gated, weights):
    rows, width = gated.shape
    return pl.pallas_call(
        inner_kernel,
        out_shape=jax.ShapeDtypeStruct(gated.shape, jnp.float32),
        in_specs=[SMEM] * 3 + [VMEM] * 2,
        out_specs=VMEM,
        scratch_shapes=[pltpu.VMEM((width // LANES, rows + 2 * RIM, LANES), jnp.float32)],
        compiler_params=pltpu.CompilerParams(vmem_limit_bytes=16 * 1024 * 1024),
    )(me, starts, ends, gated, weights)


def last_kernel(
    me, start_ref, end_ref, inner, left, right, residual, weights, gain, w_proj_hbm, out, *scratch
):
    w_proj, total, edge, sem = scratch
    copy = pltpu.make_async_copy(w_proj_hbm, w_proj, sem)
    copy.start()
    rows, width = inner.shape
    total[...] = inner[...]
    count = weights.shape[0]
    for side, rim in enumerate((left, right)):
        at = 0 if side == 0 else 2 * RIM
        row = 0 if side == 0 else rows - ROWS
        for c in range(width // LANES):
            edge[c] = jnp.zeros(edge.shape[1:], jnp.float32)
            edge[c, at : at + RIM] = rim[:, c * LANES : (c + 1) * LANES].astype(jnp.float32)
        span = (0, RIM - 1) if side == 0 else (RIM, count)
        parts = convolve(
            edge, 0, weights, *span, me[FIRST] + row, start_ref, end_ref, True
        )
        for c, part in enumerate(parts):
            lanes = slice(c * LANES, (c + 1) * LANES)
            total[row : row + ROWS, lanes] = total[row : row + ROWS, lanes] + part
    normed = normalize(total[...], gain[0:1, :])
    activated = (normed * jax.nn.sigmoid(normed)).astype(jnp.bfloat16)
    copy.wait()
    projected = jnp.dot(activated, w_proj[...], preferred_element_type=jnp.float32)
    out[...] = (residual[...].astype(jnp.float32) + projected).astype(jnp.bfloat16)


def finish_block(me, starts, ends, inner, left, right, residual, weights, gain, w_proj):
    _, width = inner.shape
    return pl.pallas_call(
        last_kernel,
        out_shape=jax.ShapeDtypeStruct(residual.shape, jnp.bfloat16),
        in_specs=[SMEM] * 3 + [VMEM] * 6 + [HBM],
        out_specs=VMEM,
        scratch_shapes=[
            pltpu.VMEM(w_proj.shape, jnp.bfloat16),
            pltpu.VMEM(inner.shape, jnp.float32),
            pltpu.VMEM((width // LANES, 3 * RIM, LANES), jnp.float32),
            pltpu.SemaphoreType.DMA,
        ],
        compiler_params=pltpu.CompilerParams(vmem_limit_bytes=24 * 1024 * 1024),
    )(me, starts, ends, inner, left, right, residual, weights, gain, w_proj)


def body(
    frames, utt_lengths, attn_gain, w_qkv, w_out, conv_gain, w_glu, w_depth, depth_gain, w_proj
):
    frame_rows = frames.shape[1]
    block_index = lax.axis_index("blk")
    group_index = lax.axis_index("grp")
    z, yl = block_index // 2, block_index % 2
    x, core = group_index // 4, group_index % 2
    window_start = group_index * (16 * frame_rows)
    first_frame = window_start + block_index * frame_rows
    local_frames = frames[0]
    me = jnp.stack([x, core, z, yl, window_start, first_frame]).astype(jnp.int32)

    shard = w_qkv.T

    def route(offset):
        return lambda x, yh, c, z, yl: (
            (x - offset, yh, yh, z, c) if yl == c else (x - offset, 1 - yh, yh, z, c)
        )

    swap = lambda x, yh, c, z, yl: (x, yh, 1 - c, z, yl)
    across = lambda x, yh, c, z, yl: (x, yh, c, z, 1 - yl)
    near = [send(shard, route(o)) for o in OFFSETS]
    own = norm(local_frames, attn_gain[None, :])
    other = send(own, across)
    far = [send(piece, swap) for piece in near]
    stream = (me, own, other, near + far)
    key_value = project_key_value(*stream)
    piece = (frame_rows, LANES)
    queries = project(query_kernel, [piece] * 8, [(8,) + piece], *stream)
    groups = [[2 * z + yl for z in range(8)] for yl in range(2)]
    key_value = lax.all_to_all(key_value, "blk", 0, 0, axis_index_groups=groups, tiled=True)
    queries = list(queries)
    for d in SEND_ORDER:
        queries[d] = send(queries[d], lambda x, yh, c, z, yl: (x, yh, c, z + d, yl))
    ends = jnp.cumsum(utt_lengths)
    starts = ends - utt_lengths
    mixed = jnp.zeros((16, HEAD, frame_rows), jnp.bfloat16)
    for pieces in PIECES:
        ready = [queries[d] for d in pieces]
        mixed = attend(pieces, me, starts, ends, key_value, mixed, ready)
    mixed = lax.all_to_all(mixed, "blk", 0, 0, tiled=True)
    residual, gated = gate(mixed, local_frames, conv_gain[None, :], w_out, w_glu)

    def neighbour(step):
        def target(x, yh, c, z, yl):
            place = (x * 4 + yh * 2 + c) * 16 + z * 2 + yl + step
            return (place % 16) * 16 + place // 16 if 0 <= place < 256 else None

        return target

    left = send(gated[frame_rows - RIM :], neighbour(1))
    right = send(gated[:RIM], neighbour(-1))
    where = (me, starts, ends)
    inner = convolve_inner(*where, gated, w_depth)
    result = finish_block(*where, inner, left, right, residual, w_depth, depth_gain[None, :], w_proj)
    return result[None]


def solution(mesh):
    in_specs = (P("grp", "blk", None), P(), P(), P(None, "grp"), P(), P(), P(), P(), P(), P())
    out_specs = P("grp", "blk", None)
    return jax.shard_map(body, mesh=mesh, in_specs=in_specs, out_specs=out_specs, check_vma=False)
```

```python
import functools

import jax
import jax.numpy as jnp
from jax import lax
from jax.experimental import pallas as pl
from jax.experimental.pallas import tpu as pltpu
from jax.sharding import PartitionSpec as P


HEAD = 64
LANES = 128
KEY_CHUNK = 512
RIM = 16
ROWS = 16
OFFSETS = (0, 1, 3, 2)
SEND_ORDER = (1, 7, 2, 6, 3, 5, 4)
PIECES = ((0, 1, 7), (2, 6, 3, 5, 4))
LOG2E = 1.4426950408889634

epsilon = 1e-05
big_negative = -1e30


VMEM = pl.BlockSpec(memory_space=pltpu.VMEM)
SMEM = pl.BlockSpec(memory_space=pltpu.SMEM)
HBM = pl.BlockSpec(memory_space=pltpu.HBM)


def coords(index):
    b, g = divmod(index, 16)
    return g // 4, (g // 2) % 2, g % 2, b // 2, b % 2


def flat(x, yh, core, z, yl):
    return ((z % 8) * 2 + yl) * 16 + (x % 4) * 4 + yh * 2 + core


def send(value, target):
    pairs = []
    for source in range(256):
        to = target(*coords(source))
        if to is not None:
            pairs.append((source, to if isinstance(to, int) else flat(*to)))
    return lax.ppermute(value, ("blk", "grp"), pairs)


def normalize(values, row_gain):
    center = values - jnp.mean(values, axis=-1, keepdims=True)
    spread = jnp.mean(center * center, axis=-1, keepdims=True)
    return center * lax.rsqrt(spread + epsilon) * row_gain


def low_lanes(rows):
    return lax.broadcasted_iota(jnp.int32, (rows, LANES), 1) < HEAD


def swap_lanes(values):
    return pltpu.roll(values, HEAD, 1)


X, CORE, Z, YL, WINDOW, FIRST = range(6)


def shard_head(me, i):
    core = me[CORE] if i < 4 else 1 - me[CORE]
    return 2 * lax.rem(me[X] + OFFSETS[i % 4], 4) + core


def inside(position, start_ref, end_ref, place):
    start, end = jnp.zeros_like(position), jnp.zeros_like(position)
    for u in range(start_ref.shape[0]):
        start, end = jnp.where(place == u, start_ref[u], start), jnp.where(place == u, end_ref[u], end)
    return (position >= start) & (position < end)


CONTRACT = (((1,), (1,)), ((), ()))


def transposed(out, index, start, flipped):
    for j in range(flipped.shape[1] // LANES):
        at = start + j * HEAD
        out[index, at : at + HEAD] = flipped[:, j * LANES : (j + 1) * LANES].astype(jnp.bfloat16)


def norm_kernel(frames, gain, out):
    out[...] = normalize(frames[...].astype(jnp.float32), gain[0:1, :]).astype(jnp.bfloat16)


def norm(frames, gain):
    return pl.pallas_call(
        norm_kernel,
        out_shape=jax.ShapeDtypeStruct(frames.shape, jnp.bfloat16),
        in_specs=[VMEM] * 2,
        out_specs=VMEM,
        compiler_params=pltpu.CompilerParams(vmem_limit_bytes=8 * 1024 * 1024),
    )(frames, gain)


def key_value_kernel(me, own, other, *refs):
    near, far_hbm, out_hbm, stream, far, out, sems, out_sems = refs[:4], refs[4:8], *refs[8:]
    copies = [pltpu.make_async_copy(far_hbm[i], far.at[i], sems.at[i]) for i in range(4)]
    for copy in copies:
        copy.start()
    rows = own.shape[0]
    stream[:rows] = own[...]
    stream[rows:] = other[...]
    low = low_lanes(rows)
    leaving = []
    for first, part in ((0, near), (4, [far.at[i] for i in range(4)])):
        if first:
            for copy in copies:
                copy.wait()
        heads = [shard_head(me, first + j) for j in range(4)]
        weights = jnp.concatenate([shard[:HEAD, :] for shard in part], axis=0)
        both = lax.dot_general(stream[...], weights, CONTRACT, preferred_element_type=jnp.float32)
        for j in (0, 2):
            pair = both[:, j * HEAD : (j + 2) * HEAD]
            mine, theirs = pair[:rows], pair[rows:]
            out[first + j, :rows] = jnp.where(low, mine, swap_lanes(theirs)).astype(jnp.bfloat16)
            out[first + j + 1, :rows] = jnp.where(low, swap_lanes(mine), theirs).astype(jnp.bfloat16)
        weights = jnp.concatenate([shard[HEAD:, :] for shard in part], axis=0)
        both = lax.dot_general(weights, stream[...], CONTRACT, preferred_element_type=jnp.float32)
        for j in range(4):
            i = first + j
            transposed(out, i, rows, both[j * HEAD : (j + 1) * HEAD])
            leaving.append(pltpu.make_async_copy(out.at[i], out_hbm.at[heads[j]], out_sems.at[i]))
            leaving[-1].start()
    for copy in leaving:
        copy.wait()


def project_key_value(me, own, other, shards):
    rows, width = own.shape
    shape = (8, 2 * rows, LANES)
    return pl.pallas_call(
        key_value_kernel,
        out_shape=jax.ShapeDtypeStruct(shape, jnp.bfloat16),
        in_specs=[SMEM] + [VMEM] * 6 + [HBM] * 4,
        out_specs=HBM,
        scratch_shapes=[
            pltpu.VMEM((2 * rows, width), jnp.bfloat16),
            pltpu.VMEM((4,) + shards[0].shape, jnp.bfloat16),
            pltpu.VMEM(shape, jnp.bfloat16),
            pltpu.SemaphoreType.DMA((4,)),
            pltpu.SemaphoreType.DMA((8,)),
        ],
        compiler_params=pltpu.CompilerParams(vmem_limit_bytes=16 * 1024 * 1024),
    )(me, own, other, *shards)


def query_kernel(me, own, other, *refs):
    near, far, pieces, both_rows, staged = refs[:4], refs[4], refs[5:13], refs[13], refs[14]
    rows = own.shape[0]
    both_rows[:rows] = own[...]
    both_rows[rows:] = other[...]
    weights = jnp.concatenate([ref[...] for ref in near] + [far[...]], axis=0)
    both = lax.dot_general(weights, both_rows[...], CONTRACT, preferred_element_type=jnp.float32)
    both = both * (HEAD**-0.5 * LOG2E)
    for i in range(8):
        piece = lax.rem(shard_head(me, i) + 8 - me[Z], 8)
        transposed(staged, piece, 0, both[i * HEAD : (i + 1) * HEAD])
    for d in range(8):
        pieces[d][...] = staged[d]


def project(kernel, shapes, staged, me, own, other, shards):
    rows, width = own.shape
    return pl.pallas_call(
        kernel,
        out_shape=[jax.ShapeDtypeStruct(shape, jnp.bfloat16) for shape in shapes],
        in_specs=[SMEM] + [VMEM] * (2 + len(shards)),
        out_specs=[VMEM] * len(shapes),
        scratch_shapes=[pltpu.VMEM((2 * rows, width), jnp.bfloat16)]
        + [pltpu.VMEM(shape, jnp.bfloat16) for shape in staged],
        compiler_params=pltpu.CompilerParams(vmem_limit_bytes=16 * 1024 * 1024),
    )(me, own, other, *shards)


def attend_kernel(pieces, me, start_ref, end_ref, in_ref, before, *refs):
    count = len(pieces)
    parts_hbm, out_ref = refs[:count], refs[count]
    keys, values, queries, scores, most_ref, parts_q, sems = refs[count + 1 :]
    copies = [pltpu.make_async_copy(parts_hbm[d], parts_q.at[d], sems.at[d]) for d in range(count)]
    for copy in copies:
        copy.start()
    out_ref[...] = before[...]
    sources = in_ref.shape[0]
    block = in_ref.shape[1] // 2
    low = low_lanes(block)
    row = lax.broadcasted_iota(jnp.int32, (block, LANES), 0)
    lane = lax.broadcasted_iota(jnp.int32, (block, LANES), 1) - HEAD
    place = lax.broadcasted_iota(jnp.int32, (16, block), 0)
    column = lax.broadcasted_iota(jnp.int32, (16, block), 1)
    window = keys.shape[0]
    top = lax.broadcasted_iota(jnp.int32, (values.shape[1] - HEAD, KEY_CHUNK), 0) == 0
    for j in range(values.shape[0]):
        values[j, HEAD:] = jnp.where(top, 1.0, 0.0).astype(jnp.bfloat16)

    def prepare(s, carry):
        key = in_ref[s, :block].astype(jnp.float32)
        for side in range(2):
            shard = 2 * s + (me[YL] if side == 0 else 1 - me[YL])
            base = me[WINDOW] + shard * block
            at = pl.ds(pl.multiple_of((2 * s + side) * block, block), block)
            mask = jnp.where(inside(row + base, start_ref, end_ref, lane), 0.0, big_negative)
            keys[at, :] = jnp.where(low, swap_lanes(key) if side else key, mask).astype(jnp.bfloat16)
        for i in range(2 * block // LANES):
            at = block + i * HEAD
            values[s, :HEAD, i * LANES : (i + 1) * LANES] = in_ref[s, at : at + HEAD]
        return carry

    def origin(i):
        side, d = lax.rem(i, 2), pieces[0]
        for j in range(1, count):
            d = jnp.where(i // 2 == j, pieces[j], d)
        shard = jnp.where(side == 0, me[YL], 1 - me[YL])
        return 2 * lax.rem(me[Z] + 8 - d, 8) + shard

    for i in range(2 * count):
        if i % 2 == 0:
            copies[i // 2].wait()
        mark = inside(column + (me[WINDOW] + origin(i) * block), start_ref, end_ref, place)
        queries[i, HEAD : HEAD + 16] = jnp.where(mark, 1.0, 0.0).astype(jnp.bfloat16)
        queries[i, HEAD + 16 :] = jnp.zeros((HEAD - 16, block), jnp.bfloat16)
        for j in range(block // LANES):
            at = ((i % 2) * (block // LANES) + j) * HEAD
            queries[i, :HEAD, j * LANES : (j + 1) * LANES] = parts_q[i // 2, at : at + HEAD]
    lax.fori_loop(0, sources, prepare, 0)
    chunks = window // KEY_CHUNK

    def score(query, j):
        at = slice(j * KEY_CHUNK, (j + 1) * KEY_CHUNK)
        return jnp.dot(keys[at, :], query, preferred_element_type=jnp.float32)

    def weigh(j, most):
        probs = jnp.exp2(scores[j * KEY_CHUNK : (j + 1) * KEY_CHUNK, :] - most)
        return jnp.dot(values[j], probs.astype(jnp.bfloat16), preferred_element_type=jnp.float32)

    def finish(total, i):
        mixed = total[:HEAD] / total[HEAD : HEAD + 1]
        out_ref[origin(i)] = mixed.astype(jnp.bfloat16)

    def keep(j, part, best):
        scores[j * KEY_CHUNK : (j + 1) * KEY_CHUNK, :] = part
        part = jnp.max(part.reshape(KEY_CHUNK // 8, 8, block), axis=0)
        return part if best is None else jnp.maximum(best, part)

    def settle(best):
        most_ref[...] = jnp.broadcast_to(jnp.max(best, axis=0, keepdims=True), (8, block))

    best = None
    for j in range(chunks):
        best = keep(j, score(queries[0], j), best)
    settle(best)

    def step(i, carry):
        query = queries[i]
        most = most_ref[0:1, :]
        best, total = None, None
        for j in range(chunks):
            part = weigh(j, most)
            total = part if total is None else total + part
            best = keep(j, score(query, j), best)
        settle(best)
        finish(total, i - 1)
        return carry

    lax.fori_loop(1, 2 * count, step, 0)
    total = None
    for j in range(chunks):
        part = weigh(j, most_ref[0:1, :])
        total = part if total is None else total + part
    finish(total, 2 * count - 1)


def attend(pieces, me, starts, ends, key_value, before, queries):
    sources, block = key_value.shape[0], key_value.shape[1] // 2
    window, count = 2 * block * sources, len(pieces)
    return pl.pallas_call(
        functools.partial(attend_kernel, pieces),
        out_shape=jax.ShapeDtypeStruct((2 * sources, HEAD, block), jnp.bfloat16),
        in_specs=[SMEM] * 3 + [VMEM] * 2 + [HBM] * count,
        out_specs=VMEM,
        scratch_shapes=[
            pltpu.VMEM((window, LANES), jnp.bfloat16),
            pltpu.VMEM((window // KEY_CHUNK, HEAD + 16, KEY_CHUNK), jnp.bfloat16),
            pltpu.VMEM((2 * count, LANES, block), jnp.bfloat16),
            pltpu.VMEM((window, block), jnp.float32),
            pltpu.VMEM((8, block), jnp.float32),
            pltpu.VMEM((count, block, LANES), jnp.bfloat16),
            pltpu.SemaphoreType.DMA((count,)),
        ],
        compiler_params=pltpu.CompilerParams(vmem_limit_bytes=24 * 1024 * 1024),
    )(me, starts, ends, key_value, before, *queries)


def gate_kernel(mixed, frames, gain, w_out_hbm, w_glu_hbm, residual_ref, gated_ref, *scratch):
    w_out, w_glu, attended, out_sem, glu_sem = scratch
    out_copy = pltpu.make_async_copy(w_out_hbm, w_out, out_sem)
    glu_copy = pltpu.make_async_copy(w_glu_hbm, w_glu, glu_sem)
    out_copy.start()
    glu_copy.start()
    heads = mixed.shape[0]
    for pair in range(heads // 2):
        flipped = jnp.concatenate([mixed[2 * pair], mixed[2 * pair + 1]], axis=0).astype(jnp.float32)
        attended[:, pair * LANES : (pair + 1) * LANES] = flipped.T.astype(jnp.bfloat16)
    out_copy.wait()
    projected = jnp.dot(attended[...], w_out[...], preferred_element_type=jnp.float32)
    residual = (frames[...].astype(jnp.float32) + projected).astype(jnp.bfloat16)
    residual_ref[...] = residual
    width = frames.shape[1]
    conv_in = normalize(residual.astype(jnp.float32), gain[0:1, :]).astype(jnp.bfloat16)
    glu_copy.wait()
    step = 256
    for j in range(0, width, step):
        a = jnp.dot(conv_in, w_glu[:, j : j + step], preferred_element_type=jnp.float32)
        b = jnp.dot(conv_in, w_glu[:, width + j : width + j + step], preferred_element_type=jnp.float32)
        gated_ref[:, j : j + step] = (a * jax.nn.sigmoid(b)).astype(jnp.bfloat16)


def gate(mixed, frames, gain, w_out, w_glu):
    shape = jax.ShapeDtypeStruct(frames.shape, jnp.bfloat16)
    return pl.pallas_call(
        gate_kernel,
        out_shape=[shape, shape],
        in_specs=[VMEM] * 3 + [HBM] * 2,
        out_specs=[VMEM] * 2,
        scratch_shapes=[
            pltpu.VMEM(w_out.shape, jnp.bfloat16),
            pltpu.VMEM(w_glu.shape, jnp.bfloat16),
            pltpu.VMEM(frames.shape, jnp.bfloat16),
            pltpu.SemaphoreType.DMA,
            pltpu.SemaphoreType.DMA,
        ],
        compiler_params=pltpu.CompilerParams(vmem_limit_bytes=24 * 1024 * 1024),
    )(mixed, frames, gain, w_out, w_glu)


def convolve(source, row, weights, t_first, t_last, position, start_ref, end_ref, masked):
    place = lax.broadcasted_iota(jnp.int32, (ROWS, LANES), 0) + position
    lo, hi = jnp.zeros_like(place), jnp.zeros_like(place)
    if masked:
        for u in range(start_ref.shape[0]):
            inside = (place >= start_ref[u]) & (place < end_ref[u])
            lo, hi = jnp.where(inside, start_ref[u], lo), jnp.where(inside, end_ref[u], hi)
        lo, hi = lo - place, hi - place
    tiles = source.shape[0]
    totals = [None] * tiles
    for t in range(t_first, t_last):
        same = (lo <= t - RIM + 1) & (hi > t - RIM + 1) if masked else None
        for c in range(tiles):
            term = source[c, pl.ds(row + t + 1, ROWS), :] * weights[t : t + 1, c * LANES : (c + 1) * LANES]
            term = jnp.where(same, term, 0.0) if masked else term
            totals[c] = term if totals[c] is None else totals[c] + term
    return totals


def inner_kernel(me, start_ref, end_ref, gated, weights, out, padded):
    rows, width = gated.shape
    for c in range(width // LANES):
        padded[c, :RIM] = jnp.zeros((RIM, LANES), jnp.float32)
        padded[c, RIM : RIM + rows] = gated[:, c * LANES : (c + 1) * LANES].astype(jnp.float32)
        padded[c, RIM + rows :] = jnp.zeros((RIM, LANES), jnp.float32)

    def step(i, carry):
        row = pl.multiple_of(i * ROWS, ROWS)
        position = me[FIRST] + row
        crossed = False
        for u in range(1, start_ref.shape[0]):
            crossed |= (start_ref[u] > position - RIM) & (start_ref[u] < position + ROWS + RIM)

        def run(masked):
            totals = convolve(
                padded, row, weights, 0, weights.shape[0], position, start_ref, end_ref, masked
            )
            for c, total in enumerate(totals):
                out[pl.ds(row, ROWS), c * LANES : (c + 1) * LANES] = total

        pl.when(crossed)(lambda: run(True))
        pl.when(jnp.logical_not(crossed))(lambda: run(False))
        return carry

    lax.fori_loop(0, rows // ROWS, step, 0)


def convolve_inner(me, starts, ends, gated, weights):
    rows, width = gated.shape
    return pl.pallas_call(
        inner_kernel,
        out_shape=jax.ShapeDtypeStruct(gated.shape, jnp.float32),
        in_specs=[SMEM] * 3 + [VMEM] * 2,
        out_specs=VMEM,
        scratch_shapes=[pltpu.VMEM((width // LANES, rows + 2 * RIM, LANES), jnp.float32)],
        compiler_params=pltpu.CompilerParams(vmem_limit_bytes=16 * 1024 * 1024),
    )(me, starts, ends, gated, weights)


def last_kernel(
    me, start_ref, end_ref, inner, left, right, residual, weights, gain, w_proj_hbm, out, *scratch
):
    w_proj, total, edge, sem = scratch
    copy = pltpu.make_async_copy(w_proj_hbm, w_proj, sem)
    copy.start()
    rows, width = inner.shape
    total[...] = inner[...]
    count = weights.shape[0]
    for side, rim in enumerate((left, right)):
        at = 0 if side == 0 else 2 * RIM
        row = 0 if side == 0 else rows - ROWS
        for c in range(width // LANES):
            edge[c] = jnp.zeros(edge.shape[1:], jnp.float32)
            edge[c, at : at + RIM] = rim[:, c * LANES : (c + 1) * LANES].astype(jnp.float32)
        span = (0, RIM - 1) if side == 0 else (RIM, count)
        parts = convolve(
            edge, 0, weights, *span, me[FIRST] + row, start_ref, end_ref, True
        )
        for c, part in enumerate(parts):
            lanes = slice(c * LANES, (c + 1) * LANES)
            total[row : row + ROWS, lanes] = total[row : row + ROWS, lanes] + part
    normed = normalize(total[...], gain[0:1, :])
    activated = (normed * jax.nn.sigmoid(normed)).astype(jnp.bfloat16)
    copy.wait()
    projected = jnp.dot(activated, w_proj[...], preferred_element_type=jnp.float32)
    out[...] = (residual[...].astype(jnp.float32) + projected).astype(jnp.bfloat16)


def finish_block(me, starts, ends, inner, left, right, residual, weights, gain, w_proj):
    _, width = inner.shape
    return pl.pallas_call(
        last_kernel,
        out_shape=jax.ShapeDtypeStruct(residual.shape, jnp.bfloat16),
        in_specs=[SMEM] * 3 + [VMEM] * 6 + [HBM],
        out_specs=VMEM,
        scratch_shapes=[
            pltpu.VMEM(w_proj.shape, jnp.bfloat16),
            pltpu.VMEM(inner.shape, jnp.float32),
            pltpu.VMEM((width // LANES, 3 * RIM, LANES), jnp.float32),
            pltpu.SemaphoreType.DMA,
        ],
        compiler_params=pltpu.CompilerParams(vmem_limit_bytes=24 * 1024 * 1024),
    )(me, starts, ends, inner, left, right, residual, weights, gain, w_proj)


def body(
    frames, utt_lengths, attn_gain, w_qkv, w_out, conv_gain, w_glu, w_depth, depth_gain, w_proj
):
    frame_rows = frames.shape[1]
    block_index = lax.axis_index("blk")
    group_index = lax.axis_index("grp")
    z, yl = block_index // 2, block_index % 2
    x, core = group_index // 4, group_index % 2
    window_start = group_index * (16 * frame_rows)
    first_frame = window_start + block_index * frame_rows
    local_frames = frames[0]
    me = jnp.stack([x, core, z, yl, window_start, first_frame]).astype(jnp.int32)

    shard = w_qkv.T

    def route(offset):
        return lambda x, yh, c, z, yl: (
            (x - offset, yh, yh, z, c) if yl == c else (x - offset, 1 - yh, yh, z, c)
        )

    swap = lambda x, yh, c, z, yl: (x, yh, 1 - c, z, yl)
    across = lambda x, yh, c, z, yl: (x, yh, c, z, 1 - yl)
    near = [send(shard[HEAD:], route(o)) for o in OFFSETS]
    near_q = [send(shard[:HEAD], route(o)) for o in OFFSETS]
    far_q = send(jnp.concatenate(near_q, axis=0), swap)
    own = norm(local_frames, attn_gain[None, :])
    other = send(own, across)
    far = [send(piece, swap) for piece in near]
    stream = (me, own, other)
    key_value = project_key_value(*stream, near + far)
    piece = (frame_rows, LANES)
    queries = project(query_kernel, [piece] * 8, [(8,) + piece], *stream, near_q + [far_q])
    groups = [[2 * z + yl for z in range(8)] for yl in range(2)]
    key_value = lax.all_to_all(key_value, "blk", 0, 0, axis_index_groups=groups, tiled=True)
    queries = list(queries)
    for d in SEND_ORDER:
        queries[d] = send(queries[d], lambda x, yh, c, z, yl: (x, yh, c, z + d, yl))
    ends = jnp.cumsum(utt_lengths)
    starts = ends - utt_lengths
    mixed = jnp.zeros((16, HEAD, frame_rows), jnp.bfloat16)
    for pieces in PIECES:
        ready = [queries[d] for d in pieces]
        mixed = attend(pieces, me, starts, ends, key_value, mixed, ready)
    mixed = lax.all_to_all(mixed, "blk", 0, 0, tiled=True)
    residual, gated = gate(mixed, local_frames, conv_gain[None, :], w_out, w_glu)

    def neighbour(step):
        def target(x, yh, c, z, yl):
            place = (x * 4 + yh * 2 + c) * 16 + z * 2 + yl + step
            return (place % 16) * 16 + place // 16 if 0 <= place < 256 else None

        return target

    left = send(gated[frame_rows - RIM :], neighbour(1))
    right = send(gated[:RIM], neighbour(-1))
    where = (me, starts, ends)
    inner = convolve_inner(*where, gated, w_depth)
    result = finish_block(*where, inner, left, right, residual, w_depth, depth_gain[None, :], w_proj)
    return result[None]


def solution(mesh):
    in_specs = (P("grp", "blk", None), P(), P(), P(None, "grp"), P(), P(), P(), P(), P(), P())
    out_specs = P("grp", "blk", None)
    return jax.shard_map(body, mesh=mesh, in_specs=in_specs, out_specs=out_specs, check_vma=False)
```
